128 devices in a mesh: dom: 32 (over x, y, core), shift: 4 (over z).
Axes of the slice: x: 4, y: 4, z: 4, core: 2. Of those that a mesh axis runs over, the one named last changes fastest.
Arguments:
- sources: float32 [32, 128, 16, 128], P('shift', 'dom'), may hold values from -6 to 6
- kappa: float32 [128, 16, 128], P('dom'), may hold values from 0 to 2
- mass: float32 [128, 16, 128], P('dom'), may hold values from 0.25 to 4
- shift_table: float32 [64], replicated, may hold values from 0.5 to 4
- shift_ids: int32 [16], P('shift'), may hold values from 0 to 63
- sketch: bfloat16 [1024, 128, 16, 128], P(None, 'dom'), may hold values from -0.1875 to 0.1875
Outputs:
- solution: float32 [16, 32, 128, 16, 128], P('shift', None, 'dom')
- residual: float32 [16, 32, 128, 16, 128], P('shift', None, 'dom')
The draws below stay inside these ranges and needn't reach their ends.
Inputs may be any that keep to these rules, and one draw needn't show every extreme that they name: `shift_ids`: index into shift_table.
All inputs are finite; a program needn't handle non-finite values.
Results may differ from the reference program's by a relative error of at most 0.0026.
Values sent between devices are 32-bit elements; how exact they have to be, the bound alone decides.
A program may use at most 128 MiB of HBM per device.

```python
import math
import jax
import jax.numpy as jnp
from jax import lax

SK = 1024
SHIFTS = 16
TABLE = 64
NY = 16
NZ = 128
B = 32
NX = 128


def plant(array, stream_key, least, top_value):
    dims = array.shape
    place = [jax.random.randint(jax.random.fold_in(stream_key, axis), (), 0, dims[axis]) for axis in range(len(dims))]
    array = array.at[tuple(place)].set(least)
    longest = dims.index(max(dims))
    place[longest] = (place[longest] + 1) % dims[longest]
    return array.at[tuple(place)].set(top_value)


def block_scale(own_key, shape, cuts, least, largest):
    gain, own = 1.0, jax.random.fold_in(own_key, 6)
    for dim, blocks in cuts:
        steps = jnp.exp(jax.random.uniform(jax.random.fold_in(own, dim), (blocks,), jnp.float32, least / len(cuts), largest / len(cuts)))
        gain = gain * jnp.repeat(steps, shape[dim] // blocks).reshape([-1 if axis == dim else 1 for axis in range(len(shape))])
    return gain


def gaussian(key, shape, deviation, reach, pieces=(), held_as=jnp.bfloat16):
    drawn = jax.random.normal(key, shape, jnp.float32) * deviation
    if len(pieces) > 0:
        drawn = block_scale(key, shape, pieces, -0.22, 0.18) * drawn
    return jnp.clip(drawn, min=-reach, max=reach).astype(held_as)


def setup_inputs(seed: int = 0) -> dict:
    splits = jax.random.split(jax.random.key(seed), 7)
    return {
        "sources": gaussian(splits[0], (B, NX, NY, NZ), 1.0, 6.0, ((0, 4), (1, 32)), jnp.float32),
        "kappa": jnp.clip(2.0 * jax.random.uniform(splits[1], (NX, NY, NZ), jnp.float32) ** block_scale(splits[1], (NX, NY, NZ), ((0, 32),), -0.2, 0.2), 0.0, 2.0),
        "mass": jnp.clip(jnp.exp(math.log(4.0) - 2.7725887 * jax.random.uniform(splits[2], (NX, NY, NZ), jnp.float32) ** block_scale(splits[2], (NX, NY, NZ), ((0, 32),), -0.2, 0.2)), 0.25, 4.0),
        "shift_table": jnp.clip(jax.random.uniform(splits[3], (TABLE,), jnp.float32, 0.5, 4.0), 0.5, 4.0),
        "shift_ids": plant(jax.random.randint(splits[4], (SHIFTS,), 0, TABLE), jax.random.fold_in(splits[4], 1), 0, TABLE - 1).astype(jnp.int32),
        "sketch": gaussian(splits[5], (SK, NX, NY, NZ), SK ** -0.5, 0.1875, ((1, 32),)),
    }


def shift_values(shift_table, shift_ids):
    entries = jnp.arange(shift_table.shape[0], dtype=jnp.int32)
    picked = jnp.where(shift_ids[:, None] == entries[None, :], shift_table[None, :], 0.0)
    return lax.optimization_barrier(jnp.sum(picked, axis=1))

def apply_operator(field, diag):
    padded = jnp.pad(field, ((0, 0), (1, 1), (1, 1), (1, 1)))
    beside = padded[:, 2:, 1:-1, 1:-1] + padded[:, :-2, 1:-1, 1:-1]
    beside = beside + padded[:, 1:-1, 2:, 1:-1] + padded[:, 1:-1, :-2, 1:-1]
    beside = beside + padded[:, 1:-1, 1:-1, 2:] + padded[:, 1:-1, 1:-1, :-2]
    return diag * field - beside

def solve_small(gram):
    h_vals = [gram[:, 1 + i, 0] for i in range(3)]
    ridge = 0.001 * (gram[:, 1, 1] + gram[:, 2, 2] + gram[:, 3, 3]) / 3.0 + 1.0
    entry = [[gram[:, 1 + i, 1 + k] + (ridge if i == k else 0.0) for k in range(3)] for i in range(3)]
    l00 = jnp.sqrt(entry[0][0])
    l10 = entry[1][0] / l00
    l20 = entry[2][0] / l00
    l11 = jnp.sqrt(entry[1][1] - l10 * l10)
    l21 = (entry[2][1] - l20 * l10) / l11
    l22 = jnp.sqrt(entry[2][2] - l20 * l20 - l21 * l21)
    f0 = h_vals[0] / l00
    f1 = (h_vals[1] - l10 * f0) / l11
    f2 = (h_vals[2] - l20 * f0 - l21 * f1) / l22
    c2 = f2 / l22
    c1 = (f1 - l21 * c2) / l11
    c0 = (f0 - l10 * c1 - l20 * c2) / l00
    return (c0, c1, c2)

def gram_of(sketched):
    return jnp.einsum('rib,rkb->bik', sketched, sketched, precision=lax.Precision.HIGHEST)

def reference(sources, kappa, mass, shift_table, shift_ids, sketch):
    sigma = shift_values(shift_table, shift_ids)
    matrix = sketch.reshape(sketch.shape[0], -1)
    count = sources.shape[0]

    def one_shift(value):
        diag = (6.0 - kappa + value * mass)[None]
        center = 6.0 + value
        w0 = sources
        z0 = apply_operator(w0, diag)
        w1 = (z0 - center * w0) / 6.0
        z1 = apply_operator(w1, diag)
        w2 = (z1 - center * w1) / 6.0
        z2 = apply_operator(w2, diag)
        stacked = jnp.stack([w0, z0, z1, z2], axis=0).astype(jnp.bfloat16).reshape(4 * count, -1)
        sketched = lax.dot_general(matrix, stacked, (((1,), (1,)), ((), ())), preferred_element_type=jnp.float32)
        gram = gram_of(sketched.reshape(matrix.shape[0], 4, count))
        c0, c1, c2 = solve_small(gram)
        c0 = c0[:, None, None, None]
        c1 = c1[:, None, None, None]
        c2 = c2[:, None, None, None]
        solution = c0 * w0 + c1 * w1 + c2 * w2
        residual = w0 - c0 * z0 - c1 * z1 - c2 * z2
        return (solution, residual)
    solution, residual = lax.map(one_shift, sigma)
    return (solution, residual)
```

```python
import functools
import jax
import jax.numpy as jnp
from jax import lax
from jax.experimental import pallas as pl
from jax.experimental.pallas import tpu as pltpu
from jax.sharding import PartitionSpec as P

F32 = jnp.float32
BF16 = jnp.bfloat16
CENTER = 2.25
K0 = 6.0 + CENTER
LOW = (0, 1, 3, 4, 6, 7)
VMEM = pltpu.VMEM
ANY = pl.ANY
MiB = 1024 * 1024


def rdma(src, dst, send, recv, where):
    return pltpu.make_async_remote_copy(
        src_ref=src, dst_ref=dst, send_sem=send, recv_sem=recv,
        device_id=where, device_id_type=pl.DeviceIdType.MESH,
    )


def signal(sem, where):
    pl.semaphore_signal(sem, inc=1, device_id=where, device_id_type=pl.DeviceIdType.MESH)


def spread_kernel(doms, zs, src, kap, mas, wide, cw, loc, hs, hr, cs, cr, gs, gr):
    d, z = lax.axis_index("dom"), lax.axis_index("shift")
    up, down, far = lax.rem(z + 1, zs), lax.rem(z + zs - 1, zs), lax.rem(z + 2, zs)
    has_l, has_r = d > 0, d < doms - 1
    copies = [
        pltpu.make_async_copy(src, wide.at[z, :, pl.ds(3, 4)], loc.at[0]),
        pltpu.make_async_copy(kap, cw.at[0, pl.ds(2, 4)], loc.at[1]),
        pltpu.make_async_copy(mas, cw.at[1, pl.ds(2, 4)], loc.at[2]),
    ]
    for c in copies:
        c.start()
    bar = pltpu.get_barrier_semaphore()
    signal(bar, {"shift": up})
    signal(bar, {"shift": down})

    @pl.when(has_l)
    def _():
        signal(bar, {"dom": d - 1})

    @pl.when(has_r)
    def _():
        signal(bar, {"dom": d + 1})

    pl.semaphore_wait(bar, 2 + has_l.astype(jnp.int32) + has_r.astype(jnp.int32))

    @pl.when(d == 0)
    def _():
        for g in range(4):
            for s in range(8):
                wide[g, s, 0:3] = jnp.zeros((3, 16, 128), F32)
        cw[:, 0:2] = jnp.zeros((2, 2, 16, 128), F32)

    @pl.when(d == doms - 1)
    def _():
        for g in range(4):
            for s in range(8):
                wide[g, s, 7:10] = jnp.zeros((3, 16, 128), F32)
        cw[:, 6:8] = jnp.zeros((2, 2, 16, 128), F32)

    for c in copies:
        c.wait()

    def to_left(g):
        return rdma(wide.at[g, :, pl.ds(3, 3)], wide.at[g, :, pl.ds(7, 3)], hs.at[0, g], hr.at[0, g], {"dom": d - 1})

    def to_right(g):
        return rdma(wide.at[g, :, pl.ds(4, 3)], wide.at[g, :, pl.ds(0, 3)], hs.at[1, g], hr.at[1, g], {"dom": d + 1})

    def coeff_left():
        return rdma(cw.at[:, pl.ds(2, 2)], cw.at[:, pl.ds(6, 2)], cs.at[0], cr.at[0], {"dom": d - 1})

    def coeff_right():
        return rdma(cw.at[:, pl.ds(4, 2)], cw.at[:, pl.ds(0, 2)], cs.at[1], cr.at[1], {"dom": d + 1})

    def start_halo(g):
        @pl.when(has_l)
        def _():
            to_left(g).start()

        @pl.when(has_r)
        def _():
            to_right(g).start()

    @pl.when(has_l)
    def _():
        coeff_left().start()

    @pl.when(has_r)
    def _():
        coeff_right().start()

    start_halo(z)
    own = wide.at[z, :, pl.ds(3, 4)]
    send_up = rdma(own, own, gs.at[0], gr.at[0], {"shift": up})
    send_down = rdma(own, own, gs.at[1], gr.at[1], {"shift": down})
    send_up.start()
    send_down.start()
    send_up.wait_recv()
    half_a = wide.at[down, pl.ds(0, 4), pl.ds(3, 4)]
    relay_up = rdma(half_a, half_a, gs.at[2], gr.at[2], {"shift": up})
    relay_up.start()
    start_halo(down)
    send_down.wait_recv()
    half_b = wide.at[up, pl.ds(4, 4), pl.ds(3, 4)]
    relay_down = rdma(half_b, half_b, gs.at[3], gr.at[3], {"shift": down})
    relay_down.start()
    start_halo(up)
    relay_up.wait_recv()
    relay_down.wait_recv()
    start_halo(far)

    @pl.when(has_l)
    def _():
        coeff_left().wait_send()
        coeff_right().wait_recv()
        for g in range(4):
            to_left(g).wait_send()
            to_right(g).wait_recv()

    @pl.when(has_r)
    def _():
        coeff_right().wait_send()
        coeff_left().wait_recv()
        for g in range(4):
            to_right(g).wait_send()
            to_left(g).wait_recv()

    for c in (send_up, send_down, relay_up, relay_down):
        c.wait_send()


def neighbours(planes, i, masks):
    v = planes[i]
    first_y, last_y, first_z, last_z = masks
    beside = planes[i + 1] + planes[i - 1]
    beside = beside + jnp.where(first_y, 0.0, pltpu.roll(v, 1, 0)) + jnp.where(last_y, 0.0, pltpu.roll(v, 15, 0))
    return beside + jnp.where(first_z, 0.0, pltpu.roll(v, 1, 1)) + jnp.where(last_z, 0.0, pltpu.roll(v, 127, 1))


def make_masks():
    rows = lax.broadcasted_iota(jnp.int32, (16, 128), 0)
    lanes = lax.broadcasted_iota(jnp.int32, (16, 128), 1)
    return rows == 0, rows == 15, lanes == 0, lanes == 127


def fields_of(w, kap, mas, inside, masks):
    sixth = 1.0 / 6.0
    diag = [6.0 - kap[i] + CENTER * mas[i] for i in range(8)]

    def op(planes, i, k):
        return diag[k] * planes[i] - neighbours(planes, i, masks)

    z00, z01, p0, p1 = [], [], [], []
    for i in range(8):
        a = op(w, i + 1, i)
        b = mas[i] * w[i + 1]
        z00.append(a)
        z01.append(b)
        p0.append((a - K0 * w[i + 1]) * (sixth * inside[i]))
        p1.append((b - w[i + 1]) * sixth)
    z10, z11, z12, q0, q1, q2 = [], [], [], [], [], []
    for i in range(6):
        k = i + 1
        a = op(p0, k, k)
        b = op(p1, k, k) + mas[k] * p0[k]
        c = mas[k] * p1[k]
        z10.append(a)
        z11.append(b)
        z12.append(c)
        q0.append((a - K0 * p0[k]) * (sixth * inside[k]))
        q1.append((b - K0 * p1[k] - p0[k]) * (sixth * inside[k]))
        q2.append((c - p1[k]) * sixth)
    z20, z21, z22, z23 = [], [], [], []
    for i in range(4):
        k, n = i + 2, i + 1
        z20.append(op(q0, n, k))
        z21.append(op(q1, n, k) + mas[k] * q0[n])
        z22.append(op(q2, n, k) + mas[k] * q1[n])
        z23.append(mas[k] * q2[n])
    zs = [w[3:7], z00[2:6], z01[2:6], z10[1:5], z11[1:5], z12[1:5], z20, z21, z22, z23]
    ws = [p0[2:6], p1[2:6], q0[1:5], q1[1:5], q2[1:5]]
    return zs, ws


def inside_of(d, doms):
    out = []
    for i in range(8):
        plane = d * 4 + (i - 2)
        ok = (plane >= 0) & (plane < doms * 4)
        out.append(jnp.where(ok, 1.0, 0.0).astype(F32))
    return out


def sketch_kernel(doms, s_ref, wide, cw, out, buf, wb, cb, gb, ob, sems, loc):
    d, z = lax.axis_index("dom"), lax.axis_index("shift")
    pairs = [pltpu.make_async_copy(s_ref.at[:, q], buf.at[q], sems.at[q]) for q in range(32)]
    ins = [
        pltpu.make_async_copy(wide.at[z], wb, loc.at[0]),
        pltpu.make_async_copy(cw, cb, loc.at[1]),
    ]
    for c in ins:
        c.start()
    for c in pairs:
        c.start()
    for c in ins:
        c.wait()
    masks = make_masks()
    inside = inside_of(d, doms)
    kap = [cb[0, i] for i in range(8)]
    mas = [cb[1, i] for i in range(8)]

    def one(s, carry):
        w = [wb[s, i] for i in range(10)]
        zs, _ = fields_of(w, kap, mas, inside, masks)
        col = pl.multiple_of(s * 16, 16)
        for x in range(4):
            high = [f[x] for f in zs]
            low = [high[k] - high[k].astype(BF16).astype(F32) for k in LOW]
            stacked = jnp.stack(high + low, axis=0)
            turned = jnp.transpose(stacked, (1, 0, 2)).astype(BF16)
            for y in range(16):
                gb[x * 8 + y // 2, pl.ds((y % 2) * 128 + col, 16), :] = turned[y]
        return carry

    lax.fori_loop(0, 8, one, 0)
    for c in pairs:
        c.wait()
    rows = buf.reshape(32, 2048, 128)

    def block(i, carry):
        at = pl.multiple_of(i * 512, 512)
        lhs = jnp.concatenate([rows[q, pl.ds(at, 512), :] for q in range(32)], axis=1)
        rhs = jnp.concatenate([gb[q] for q in range(32)], axis=1)
        ob[pl.ds(at, 512), :] = lax.dot_general(lhs, rhs, (((1,), (1,)), ((), ())), preferred_element_type=F32)
        return carry

    lax.fori_loop(0, 4, block, 0)
    even = lax.broadcasted_iota(jnp.int32, (128, 128), 0) % 2 == 0
    for i in range(8):
        a = ob[128 * i : 128 * i + 128, :]
        b = ob[1024 + 128 * i : 1024 + 128 * i + 128, :]
        xa = a[:, :128] + pltpu.roll(a[:, 128:], 127, 0)
        xb = b[:, 128:] + pltpu.roll(b[:, :128], 1, 0)
        out[128 * i : 128 * i + 128, :] = jnp.where(even, xa, xb)


def gram_kernel(doms, zs, part, gall, r1, mine, r2, dm, rd, s1, e1, s2, e2, s3, e3, s4, e4):
    d, z = lax.axis_index("dom"), lax.axis_index("shift")
    core, chip, chips = lax.rem(d, 2), d // 2, doms // 2
    bar = pltpu.get_barrier_semaphore()
    for k in range(1, doms):
        signal(bar, {"dom": lax.rem(d + k, doms)})
    for k in range(1, zs):
        signal(bar, {"shift": lax.rem(z + k, zs)})
    pl.semaphore_wait(bar, doms + zs - 2)
    other = pl.multiple_of((1 - core) * 512, 512)
    keep = pl.multiple_of(core * 512, 512)
    swap = rdma(part.at[pl.ds(other, 512)], r1, s1, e1, {"dom": d + 1 - 2 * core})
    swap.start()
    swap.wait_recv()
    mine[...] = part[pl.ds(keep, 512)] + r1[...]
    sends = []
    for k in range(1, chips):
        t = lax.rem(chip + k, chips)
        c = rdma(mine.at[pl.ds(pl.multiple_of(t * 32, 32), 32)], r2.at[k], s2.at[k], e2.at[k], {"dom": 2 * t + core})
        c.start()
        sends.append(c)
    v = mine[pl.ds(pl.multiple_of(chip * 32, 32), 32)]
    for c, k in zip(sends, range(1, chips)):
        c.wait_recv()
        v = v + r2[k]
    full = lax.dot_general(v, v, (((0,), (0,)), ((), ())), precision=lax.Precision.HIGHEST, preferred_element_type=F32)
    owner = lax.broadcasted_iota(jnp.int32, (16, 128), 1) // 16
    diag = jnp.zeros((16, 128), F32)
    for s in range(8):
        diag = jnp.where(owner == s, full[16 * s : 16 * s + 16], diag)
    dm[...] = diag
    for k in range(1, doms):
        c = rdma(dm, rd.at[k], s3.at[k], e3.at[k], {"dom": lax.rem(d + k, doms)})
        c.start()
        sends.append(c)
    total = diag
    for k in range(1, doms):
        sends[chips - 2 + k].wait_recv()
        total = total + rd[k]
    gall[z] = total
    tail = []
    for k in range(1, zs):
        c = rdma(gall.at[z], gall.at[z], s4.at[k], e4.at[k], {"shift": lax.rem(z + k, zs)})
        c.start()
        tail.append(c)
    for c in tail:
        c.wait_recv()
    swap.wait_send()
    for c in sends + tail:
        c.wait_send()


def output_kernel(doms, step, coef, wide, cw, sol, res, fb):
    d = lax.axis_index("dom")
    base = pl.program_id(0) * step
    masks = make_masks()
    inside = inside_of(d, doms)
    kap = [cw[0, i] for i in range(8)]
    mas = [cw[1, i] for i in range(8)]

    def one(b, carry):
        w = [wide[b, i] for i in range(10)]
        zf, wf = fields_of(w, kap, mas, inside, masks)
        for n, f in enumerate(zf + wf):
            for x in range(4):
                fb[n, x] = f[x]

        def system(j, carry):
            at = (j * 32 + base + b) * 16
            c = [coef[at + i] for i in range(15)]
            for x in range(4):
                s = c[9] * fb[0, x]
                for n in range(10, 15):
                    s = s + c[n] * fb[n, x]
                r = fb[0, x]
                for n in range(9):
                    r = r - c[n] * fb[n + 1, x]
                sol[j, b, x] = s
                res[j, b, x] = r
            return carry

        lax.fori_loop(0, 4, system, 0)
        return carry

    lax.fori_loop(0, step, one, 0)


def shift_values(shift_table, shift_ids):
    entries = jnp.arange(shift_table.shape[0], dtype=jnp.int32)
    picked = jnp.where(shift_ids[:, None] == entries[None, :], shift_table[None, :], 0.0)
    return jnp.sum(picked, axis=1)


def solve_small(gram):
    h_vals = [gram[..., 1 + i, 0] for i in range(3)]
    ridge = 0.001 * (gram[..., 1, 1] + gram[..., 2, 2] + gram[..., 3, 3]) / 3.0 + 1.0
    entry = [[gram[..., 1 + i, 1 + k] + (ridge if i == k else 0.0) for k in range(3)] for i in range(3)]
    l00 = jnp.sqrt(entry[0][0])
    l10 = entry[1][0] / l00
    l20 = entry[2][0] / l00
    l11 = jnp.sqrt(entry[1][1] - l10 * l10)
    l21 = (entry[2][1] - l20 * l10) / l11
    l22 = jnp.sqrt(entry[2][2] - l20 * l20 - l21 * l21)
    f0 = h_vals[0] / l00
    f1 = (h_vals[1] - l10 * f0) / l11
    f2 = (h_vals[2] - l20 * f0 - l21 * f1) / l22
    c2 = f2 / l22
    c1 = (f1 - l21 * c2) / l11
    c0 = (f0 - l10 * c1 - l20 * c2) / l00
    return c0, c1, c2


def coefficients(gall, sigma):
    t = sigma - CENTER
    one, zero = jnp.ones_like(t), jnp.zeros_like(t)
    powers = [one, t, t * t, t * t * t]
    owner = [0, 1, 1, 2, 2, 2, 3, 3, 3, 3]
    degree = [0, 0, 1, 0, 1, 2, 0, 1, 2, 3]
    owner += [owner[k] for k in LOW]
    degree += [degree[k] for k in LOW]
    mix = jnp.stack(
        [jnp.stack([powers[degree[f]] if owner[f] == i else zero for f in range(16)], 1) for i in range(4)], 1
    )
    grams = gall.reshape(4, 16, 8, 16).transpose(0, 2, 1, 3).reshape(32, 16, 16)
    left = jnp.einsum("jif,bfg->jbig", mix, grams, precision=lax.Precision.HIGHEST)
    gram = jnp.einsum("jbig,jkg->jbik", left, mix, precision=lax.Precision.HIGHEST)
    c0, c1, c2 = solve_small(gram)
    t = t[:, None]
    out = [c0, c0 * t, c1, c1 * t, c1 * t * t, c2, c2 * t, c2 * t * t, c2 * t * t * t]
    out += [c0, c1, c1 * t, c2, c2 * t, c2 * t * t, jnp.zeros_like(c0)]
    return jnp.stack(out, axis=-1).reshape(-1)


def on_device(sources, kappa, mass, shift_table, shift_ids, sketch):
    doms, zs = lax.axis_size("dom"), lax.axis_size("shift")
    sds = jax.ShapeDtypeStruct
    dma = pltpu.SemaphoreType.DMA
    wide, cw = pl.pallas_call(
        functools.partial(spread_kernel, doms, zs),
        out_shape=(sds((4, 8, 10, 16, 128), F32), sds((2, 8, 16, 128), F32)),
        in_specs=[pl.BlockSpec(memory_space=ANY)] * 3,
        out_specs=(pl.BlockSpec(memory_space=VMEM), pl.BlockSpec(memory_space=VMEM)),
        scratch_shapes=[dma((3,)), dma((2, 4)), dma((2, 4)), dma((2,)), dma((2,)), dma((4,)), dma((4,))],
        compiler_params=pltpu.CompilerParams(collective_id=0, has_side_effects=True),
        name="spread",
    )(sources, kappa, mass)
    part = pl.pallas_call(
        functools.partial(sketch_kernel, doms),
        out_shape=sds((1024, 128), F32),
        in_specs=[pl.BlockSpec(memory_space=ANY)] * 3,
        out_specs=pl.BlockSpec(memory_space=VMEM),
        scratch_shapes=[
            VMEM((32, 1024, 2, 128), BF16), VMEM((8, 10, 16, 128), F32), VMEM((2, 8, 16, 128), F32),
            VMEM((32, 256, 128), BF16), VMEM((2048, 256), F32), dma((32,)), dma((2,)),
        ],
        compiler_params=pltpu.CompilerParams(vmem_limit_bytes=48 * MiB),
        name="sketch",
    )(sketch.reshape(1024, 32, 2, 128), wide, cw)
    gall = pl.pallas_call(
        functools.partial(gram_kernel, doms, zs),
        out_shape=sds((4, 16, 128), F32),
        in_specs=[pl.BlockSpec(memory_space=VMEM)],
        out_specs=pl.BlockSpec(memory_space=VMEM),
        scratch_shapes=[
            VMEM((512, 128), F32), VMEM((512, 128), F32), VMEM((16, 32, 128), F32), VMEM((16, 128), F32),
            VMEM((32, 16, 128), F32), dma, dma, dma((16,)), dma((16,)), dma((32,)), dma((32,)), dma((4,)), dma((4,)),
        ],
        compiler_params=pltpu.CompilerParams(collective_id=1, has_side_effects=True),
        name="gram",
    )(part)
    coef = coefficients(gall, shift_values(shift_table, shift_ids))
    step = 4
    out = sds((4, 32, 4, 16, 128), F32)
    out_spec = pl.BlockSpec((4, step, 4, 16, 128), lambda i: (0, i, 0, 0, 0))
    return pl.pallas_call(
        functools.partial(output_kernel, doms, step),
        out_shape=(out, out),
        grid=(32 // step,),
        in_specs=[
            pl.BlockSpec(memory_space=pltpu.SMEM),
            pl.BlockSpec((step, 10, 16, 128), lambda i: (i, 0, 0, 0)),
            pl.BlockSpec((2, 8, 16, 128), lambda i: (0, 0, 0, 0)),
        ],
        out_specs=(out_spec, out_spec),
        scratch_shapes=[VMEM((15, 4, 16, 128), F32)],
        compiler_params=pltpu.CompilerParams(vmem_limit_bytes=32 * MiB),
        name="outputs",
    )(coef, wide.reshape(32, 10, 16, 128), cw)


def solution(mesh):
    placed = (
        P("shift", "dom", None, None), P("dom", None, None), P("dom", None, None), P(), P("shift"),
        P(None, "dom", None, None),
    )
    return jax.shard_map(
        on_device,
        mesh=mesh,
        in_specs=placed,
        out_specs=(P("shift", None, "dom", None, None), P("shift", None, "dom", None, None)),
        check_vma=False,
    )
```

```python
import functools
import jax
import jax.numpy as jnp
from jax import lax
from jax.experimental import pallas as pl
from jax.experimental.pallas import tpu as pltpu
from jax.sharding import PartitionSpec as P

F32 = jnp.float32
BF16 = jnp.bfloat16
CENTER = 2.25
K0 = 6.0 + CENTER
ORDER = (0, 1, 3, 4, 6, 7, 2, 5, 8, 9)
OWNER = (0, 1, 2, 2, 3, 3, 1, 2, 3, 3)
DEGREE = (0, 0, 0, 1, 0, 1, 1, 2, 2, 3)
LOWS = 6
VMEM = pltpu.VMEM
ANY = pl.ANY
MiB = 1024 * 1024


def rdma(src, dst, send, recv, where):
    return pltpu.make_async_remote_copy(
        src_ref=src, dst_ref=dst, send_sem=send, recv_sem=recv,
        device_id=where, device_id_type=pl.DeviceIdType.MESH,
    )


def signal(sem, where):
    pl.semaphore_signal(sem, inc=1, device_id=where, device_id_type=pl.DeviceIdType.MESH)


def neighbours(planes, i, masks):
    v = planes[i]
    first_y, last_y, first_z, last_z = masks
    beside = planes[i + 1] + planes[i - 1]
    beside = beside + jnp.where(first_y, 0.0, pltpu.roll(v, 1, 0)) + jnp.where(last_y, 0.0, pltpu.roll(v, 15, 0))
    return beside + jnp.where(first_z, 0.0, pltpu.roll(v, 1, 1)) + jnp.where(last_z, 0.0, pltpu.roll(v, 127, 1))


def make_masks():
    rows = lax.broadcasted_iota(jnp.int32, (16, 128), 0)
    lanes = lax.broadcasted_iota(jnp.int32, (16, 128), 1)
    return rows == 0, rows == 15, lanes == 0, lanes == 127


def fields_of(w, kap, mas, inside, masks):
    sixth = 1.0 / 6.0
    diag = [6.0 - kap[i] + CENTER * mas[i] for i in range(8)]

    def op(planes, i, k):
        return diag[k] * planes[i] - neighbours(planes, i, masks)

    z00, z01, p0, p1 = [], [], [], []
    for i in range(8):
        a = op(w, i + 1, i)
        b = mas[i] * w[i + 1]
        z00.append(a)
        z01.append(b)
        p0.append((a - K0 * w[i + 1]) * (sixth * inside[i]))
        p1.append((b - w[i + 1]) * sixth)
    z10, z11, z12, q0, q1, q2 = [], [], [], [], [], []
    for i in range(6):
        k = i + 1
        a = op(p0, k, k)
        b = op(p1, k, k) + mas[k] * p0[k]
        c = mas[k] * p1[k]
        z10.append(a)
        z11.append(b)
        z12.append(c)
        q0.append((a - K0 * p0[k]) * (sixth * inside[k]))
        q1.append((b - K0 * p1[k] - p0[k]) * (sixth * inside[k]))
        q2.append((c - p1[k]) * sixth)
    z20, z21, z22, z23 = [], [], [], []
    for i in range(4):
        k, n = i + 2, i + 1
        z20.append(op(q0, n, k))
        z21.append(op(q1, n, k) + mas[k] * q0[n])
        z22.append(op(q2, n, k) + mas[k] * q1[n])
        z23.append(mas[k] * q2[n])
    zs = [w[3:7], z00[2:6], z01[2:6], z10[1:5], z11[1:5], z12[1:5], z20, z21, z22, z23]
    return zs


def inside_of(d, doms):
    out = []
    for i in range(8):
        plane = d * 4 + (i - 2)
        ok = (plane >= 0) & (plane < doms * 4)
        out.append(jnp.where(ok, 1.0, 0.0).astype(F32))
    return out


def small_solve(gram, h):
    ridge = 0.001 * (gram(1, 1) + gram(2, 2) + gram(3, 3)) / 3.0 + 1.0
    e00, e11, e22 = gram(1, 1) + ridge, gram(2, 2) + ridge, gram(3, 3) + ridge
    e10, e20, e21 = gram(2, 1), gram(3, 1), gram(3, 2)
    l00 = jnp.sqrt(e00)
    l10 = e10 / l00
    l20 = e20 / l00
    l11 = jnp.sqrt(e11 - l10 * l10)
    l21 = (e21 - l20 * l10) / l11
    l22 = jnp.sqrt(e22 - l20 * l20 - l21 * l21)
    f0 = h(1) / l00
    f1 = (h(2) - l10 * f0) / l11
    f2 = (h(3) - l20 * f0 - l21 * f1) / l22
    c2 = f2 / l22
    c1 = (f1 - l21 * c2) / l11
    c0 = (f0 - l10 * c1 - l20 * c2) / l00
    return c0, c1, c2


def powers_of(t):
    return [jnp.ones_like(t), t, t * t, t * t * t]


def by_lane(shape, dim_size, values, group):
    lane = lax.broadcasted_iota(jnp.int32, shape, 1)
    which = (lane % 32) // group
    out = jnp.zeros(shape, F32)
    for j, v in enumerate(values):
        out = jnp.where(which == j, v, out)
    return out


def main_kernel(
    doms, zs, table, ids, src, kap, mas, s_ref, fields, coef,
    buf, wide, cw, fb, gb, oa, ob, part, r1, mine, r2, dm, dp, ds, rd, gall,
    loc, ssem, fsem, hs, hr, cs, cr, gs, gr, s1, e1, s2, e2, s3, e3, s4, e4, s5, e5,
):
    d, z = lax.axis_index("dom"), lax.axis_index("shift")
    up, down, far = lax.rem(z + 1, zs), lax.rem(z + zs - 1, zs), lax.rem(z + 2, zs)
    core, chip, chips = lax.rem(d, 2), d // 2, doms // 2
    partner = {"dom": d + 1 - 2 * core}
    has_l, has_r = d > 0, d < doms - 1
    copies = [
        pltpu.make_async_copy(src, wide.at[z, :, pl.ds(3, 4)], loc.at[0]),
        pltpu.make_async_copy(kap, cw.at[0, pl.ds(2, 4)], loc.at[1]),
        pltpu.make_async_copy(mas, cw.at[1, pl.ds(2, 4)], loc.at[2]),
    ]
    pairs = [pltpu.make_async_copy(s_ref.at[:, q], buf.at[q], ssem.at[q]) for q in range(32)]
    for c in copies + pairs:
        c.start()
    bar = pltpu.get_barrier_semaphore()
    for k in range(1, doms):
        signal(bar, {"dom": lax.rem(d + k, doms)})
    for k in range(1, zs):
        signal(bar, {"shift": lax.rem(z + k, zs)})

    @pl.when(d == 0)
    def _():
        for g in range(4):
            for s in range(8):
                wide[g, s, 0:3] = jnp.zeros((3, 16, 128), F32)
        cw[:, 0:2] = jnp.zeros((2, 2, 16, 128), F32)

    @pl.when(d == doms - 1)
    def _():
        for g in range(4):
            for s in range(8):
                wide[g, s, 7:10] = jnp.zeros((3, 16, 128), F32)
        cw[:, 6:8] = jnp.zeros((2, 2, 16, 128), F32)

    for c in copies:
        c.wait()
    pl.semaphore_wait(bar, doms + zs - 2)

    def to_left(g):
        return rdma(wide.at[g, :, pl.ds(3, 3)], wide.at[g, :, pl.ds(7, 3)], hs.at[0, g], hr.at[0, g], {"dom": d - 1})

    def to_right(g):
        return rdma(wide.at[g, :, pl.ds(4, 3)], wide.at[g, :, pl.ds(0, 3)], hs.at[1, g], hr.at[1, g], {"dom": d + 1})

    def coeff_left():
        return rdma(cw.at[:, pl.ds(2, 2)], cw.at[:, pl.ds(6, 2)], cs.at[0], cr.at[0], {"dom": d - 1})

    def coeff_right():
        return rdma(cw.at[:, pl.ds(4, 2)], cw.at[:, pl.ds(0, 2)], cs.at[1], cr.at[1], {"dom": d + 1})

    def start_halo(g):
        @pl.when(has_l)
        def _():
            to_left(g).start()

        @pl.when(has_r)
        def _():
            to_right(g).start()

    def wait_halo(g):
        @pl.when(has_l)
        def _():
            to_right(g).wait_recv()

        @pl.when(has_r)
        def _():
            to_left(g).wait_recv()

    @pl.when(has_l)
    def _():
        coeff_left().start()

    @pl.when(has_r)
    def _():
        coeff_right().start()

    start_halo(z)
    own = wide.at[z, :, pl.ds(3, 4)]
    send_up = rdma(own, own, gs.at[0], gr.at[0], {"shift": up})
    send_down = rdma(own, own, gs.at[1], gr.at[1], {"shift": down})
    send_up.start()
    send_down.start()

    @pl.when(has_l)
    def _():
        coeff_right().wait_recv()

    @pl.when(has_r)
    def _():
        coeff_left().wait_recv()

    wait_halo(z)
    masks = make_masks()
    inside = inside_of(d, doms)

    def fields_for(g, sketched):
        def one(s, carry):
            k = [cw[0, i] for i in range(8)]
            m = [cw[1, i] for i in range(8)]
            zf = fields_of([wide[g, s, i] for i in range(10)], k, m, inside, masks)
            at = g * 8 + s
            for n in range(10):
                for x in range(4):
                    fb[at, n, x] = zf[n][x]
            if sketched:
                col = pl.multiple_of(s * 16, 16)
                for x in range(4):
                    high = [zf[n][x] for n in ORDER]
                    low = [h - h.astype(BF16).astype(F32) for h in high[:LOWS]]
                    turned = jnp.transpose(jnp.stack(high + low, axis=0), (1, 0, 2)).astype(BF16)
                    for y in range(16):
                        gb[x * 8 + y // 2, pl.ds((y % 2) * 128 + col, 16), :] = turned[y]
            return carry

        lax.fori_loop(0, 8, one, 0)

    def save(g):
        return pltpu.make_async_copy(fb.at[pl.ds(g * 8, 8)], fields.at[pl.ds(g * 8, 8)], fsem.at[g])

    fields_for(z, True)

    send_up.wait_recv()
    half_a = wide.at[down, pl.ds(0, 4), pl.ds(3, 4)]
    relay_up = rdma(half_a, half_a, gs.at[2], gr.at[2], {"shift": up})
    relay_up.start()
    send_down.wait_recv()
    half_b = wide.at[up, pl.ds(4, 4), pl.ds(3, 4)]
    relay_down = rdma(half_b, half_b, gs.at[3], gr.at[3], {"shift": down})
    relay_down.start()
    start_halo(down)
    start_halo(up)
    for c in pairs:
        c.wait()
    save(z).start()

    rows = buf.reshape(32, 2048, 128)
    even = lax.broadcasted_iota(jnp.int32, (256, 128), 0) % 2 == 0
    other = pl.multiple_of((1 - core) * 128, 128)
    keep = pl.multiple_of(core * 128, 128)

    def swap(i):
        return rdma(part.at[i, pl.ds(other, 128)], r1.at[i], s1.at[i], e1.at[i], partner)

    def scatter(i, k):
        t = lax.rem(chip + k, chips)
        return rdma(
            mine.at[i, pl.ds(pl.multiple_of(t * 8, 8), 8)], r2.at[k, i], s2.at[k, i], e2.at[k, i], {"dom": 2 * t + core}
        )

    def spread(i):
        swap(i).wait_recv()
        mine[i] = part[i, pl.ds(keep, 128)] + r1[i]
        for k in range(1, chips):
            scatter(i, k).start()

    def stage(i, carry):
        rhs = jnp.concatenate([gb[q] for q in range(32)], axis=1)
        for base, o in ((0, oa), (1024, ob)):
            at = pl.multiple_of(i * 256 + base, 256)
            lhs = jnp.concatenate([rows[q, pl.ds(at, 256), :] for q in range(32)], axis=1)
            o[...] = lax.dot_general(lhs, rhs, (((1,), (1,)), ((), ())), preferred_element_type=F32)
        a, b = oa[...], ob[...]
        xa = a[:, :128] + pltpu.roll(a[:, 128:], 255, 0)
        xb = b[:, 128:] + pltpu.roll(b[:, :128], 1, 0)
        part[i] = jnp.where(even, xa, xb)
        swap(i).start()

        @pl.when(i > 0)
        def _():
            spread(i - 1)

        return carry

    lax.fori_loop(0, 4, stage, 0)
    relay_up.wait_recv()
    relay_down.wait_recv()
    start_halo(far)
    spread(3)
    wait_halo(down)
    fields_for(down, False)

    v = []
    for i in range(4):
        total = mine[i, pl.ds(pl.multiple_of(chip * 8, 8), 8)]
        for k in range(1, chips):
            scatter(i, k).wait_recv()
            total = total + r2[k, i]
        v.append(total)
    v = jnp.concatenate(v, axis=0)
    lane = lax.broadcasted_iota(jnp.int32, (32, 128), 1) % 16
    v = v + jnp.where(lane < LOWS, pltpu.roll(v, 118, 1), 0.0)
    v = jnp.where(lane < 10, v, 0.0)
    full = lax.dot_general(v, v, (((0,), (0,)), ((), ())), precision=lax.Precision.HIGHEST, preferred_element_type=F32)
    owner = lax.broadcasted_iota(jnp.int32, (16, 128), 1) // 16
    diag = jnp.zeros((16, 128), F32)
    for s in range(8):
        diag = jnp.where(owner == s, full[16 * s : 16 * s + 16], diag)
    dm[...] = diag
    pair = rdma(dm, dp, s3, e3, partner)
    pair.start()
    save(down).start()
    pair.wait_recv()
    ds[...] = diag + dp[...]
    sums = []
    for k in range(1, chips):
        c = rdma(ds, rd.at[k], s4.at[k], e4.at[k], {"dom": 2 * lax.rem(chip + k, chips) + core})
        c.start()
        sums.append(c)
    wait_halo(up)
    fields_for(up, False)
    total = ds[...]
    for k, c in zip(range(1, chips), sums):
        c.wait_recv()
        total = total + rd[k]
    gall[z] = total
    tail = []
    for k in range(1, zs):
        c = rdma(gall.at[z], gall.at[z], s5.at[k], e5.at[k], {"shift": lax.rem(z + k, zs)})
        c.start()
        tail.append(c)
    save(up).start()
    wait_halo(far)
    fields_for(far, False)

    shifts = [table[ids[j]] - CENTER for j in range(4)]
    r = lax.broadcasted_iota(jnp.int32, (128, 128), 0)
    l = lax.broadcasted_iota(jnp.int32, (128, 128), 1)
    tw = by_lane((128, 128), 128, shifts, 8)
    pw = powers_of(tw)
    fold = jnp.zeros((128, 128), F32)
    for n in range(10):
        hit = (r % 16 == n) & (r // 16 == l % 8) & (l // 32 == OWNER[n])
        fold = jnp.where(hit, pw[DEGREE[n]], fold)
    for c in tail:
        c.wait_recv()
    mixed = lax.dot_general(
        gall[...].reshape(64, 128), fold, (((1,), (0,)), ((), ())), precision=lax.Precision.HIGHEST, preferred_element_type=F32
    )
    save(far).start()
    t = by_lane((1, 128), 128, shifts, 8)
    pt = powers_of(t)
    lines = []
    for i in range(1, 4):
        per_z = []
        for g in range(4):
            acc = jnp.zeros((1, 128), F32)
            for n in range(10):
                if OWNER[n] == i:
                    acc = acc + pt[DEGREE[n]] * mixed[g * 16 + n : g * 16 + n + 1]
            per_z.append(acc)
        lines.append(jnp.concatenate(per_z + per_z, axis=0))

    def gram(i, k):
        return lines[i - 1] if k == 0 else pltpu.roll(lines[i - 1], 128 - 32 * k, 1)

    c0, c1, c2 = small_solve(gram, lambda i: gram(i, 0))
    t = by_lane((8, 128), 128, shifts, 8)
    center = K0 + t
    sixth = 1.0 / 6.0
    e = c1 - c2 * center * sixth
    out = [c0, c0 * t, c1, c1 * t, c1 * t * t, c2, c2 * t, c2 * t * t, c2 * t * t * t]
    out += [c0 - e * center * sixth, e * sixth, e * t * sixth, c2 * sixth, c2 * t * sixth, c2 * t * t * sixth, c2]
    quarter = lax.broadcasted_iota(jnp.int32, (8, 128), 1) // 32
    for n4 in range(4):
        acc = jnp.zeros((8, 128), F32)
        for k in range(4):
            c = out[n4 * 4 + k]
            acc = jnp.where(quarter == k, c if k == 0 else pltpu.roll(c, 32 * k, 1), acc)
        coef[n4 * 8 : n4 * 8 + 8] = acc

    for i in range(4):
        swap(i).wait_send()
        for k in range(1, chips):
            scatter(i, k).wait_send()
    for c in [pair, send_up, send_down, relay_up, relay_down] + sums + tail:
        c.wait_send()

    @pl.when(has_l)
    def _():
        coeff_left().wait_send()
        for g in range(4):
            to_left(g).wait_send()

    @pl.when(has_r)
    def _():
        coeff_right().wait_send()
        for g in range(4):
            to_right(g).wait_send()

    for g in range(4):
        save(g).wait()


def output_kernel(step, coef, fields, sol, res):
    first = pl.program_id(0) * step

    def one(b, carry):
        g, s = (first + b) // 8, lax.rem(first + b, 8)
        for j in range(4):
            c = [coef[(n // 4) * 8 + g, (n % 4) * 32 + j * 8 + s] for n in range(15)]
            for x in range(4):
                f = [fields[b, n, x] for n in range(10)]
                u = c[9] * f[0]
                for n in range(1, 6):
                    u = u + c[9 + n] * f[n]
                r = f[0] - c[0] * f[1]
                for n in range(1, 9):
                    r = r - c[n] * f[n + 1]
                sol[j, b, x] = u
                res[j, b, x] = r
        return carry

    lax.fori_loop(0, step, one, 0)


def on_device(sources, kappa, mass, shift_table, shift_ids, sketch):
    doms, zs = lax.axis_size("dom"), lax.axis_size("shift")
    sds = jax.ShapeDtypeStruct
    dma = pltpu.SemaphoreType.DMA
    smem = pl.BlockSpec(memory_space=pltpu.SMEM)
    hbm = pl.BlockSpec(memory_space=ANY)
    fields, coef = pl.pallas_call(
        functools.partial(main_kernel, doms, zs),
        out_shape=(sds((32, 10, 4, 16, 128), F32), sds((32, 128), F32)),
        in_specs=[smem, smem, hbm, hbm, hbm, hbm],
        out_specs=(hbm, pl.BlockSpec(memory_space=VMEM)),
        scratch_shapes=[
            VMEM((32, 1024, 2, 128), BF16), VMEM((4, 8, 10, 16, 128), F32), VMEM((2, 8, 16, 128), F32),
            VMEM((32, 10, 4, 16, 128), F32), VMEM((32, 256, 128), BF16), VMEM((256, 256), F32), VMEM((256, 256), F32),
            VMEM((4, 256, 128), F32), VMEM((4, 128, 128), F32), VMEM((4, 128, 128), F32), VMEM((16, 4, 8, 128), F32),
            VMEM((16, 128), F32), VMEM((16, 128), F32), VMEM((16, 128), F32), VMEM((16, 16, 128), F32), VMEM((4, 16, 128), F32),
            dma((3,)), dma((32,)), dma((4,)), dma((2, 4)), dma((2, 4)), dma((2,)), dma((2,)), dma((4,)), dma((4,)),
            dma((4,)), dma((4,)), dma((16, 4)), dma((16, 4)), dma, dma, dma((16,)), dma((16,)), dma((4,)), dma((4,)),
        ],
        compiler_params=pltpu.CompilerParams(collective_id=0, has_side_effects=True, vmem_limit_bytes=56 * MiB),
        name="main",
    )(shift_table, shift_ids, sources, kappa, mass, sketch.reshape(1024, 32, 2, 128))
    step = 4
    out = sds((4, 32, 4, 16, 128), F32)
    out_spec = pl.BlockSpec((4, step, 4, 16, 128), lambda i: (0, i, 0, 0, 0))
    return pl.pallas_call(
        functools.partial(output_kernel, step),
        out_shape=(out, out),
        grid=(32 // step,),
        in_specs=[smem, pl.BlockSpec((step, 10, 4, 16, 128), lambda i: (i, 0, 0, 0, 0))],
        out_specs=(out_spec, out_spec),
        compiler_params=pltpu.CompilerParams(vmem_limit_bytes=32 * MiB),
        name="outputs",
    )(coef, fields)


def solution(mesh):
    placed = (
        P("shift", "dom", None, None), P("dom", None, None), P("dom", None, None), P(), P("shift"),
        P(None, "dom", None, None),
    )
    return jax.shard_map(
        on_device,
        mesh=mesh,
        in_specs=placed,
        out_specs=(P("shift", None, "dom", None, None), P("shift", None, "dom", None, None)),
        check_vma=False,
    )
```

```python
import functools
import jax
import jax.numpy as jnp
from jax import lax
from jax.experimental import pallas as pl
from jax.experimental.pallas import tpu as pltpu
from jax.sharding import PartitionSpec as P

F32 = jnp.float32
BF16 = jnp.bfloat16
CENTER = 2.25
K0 = 6.0 + CENTER
ORDER = (0, 1, 3, 4, 6, 7, 2, 5, 8, 9)
OWNER = (0, 1, 2, 2, 3, 3, 1, 2, 3, 3)
DEGREE = (0, 0, 0, 1, 0, 1, 1, 2, 2, 3)
LOWS = 6
VMEM = pltpu.VMEM
ANY = pl.ANY
MiB = 1024 * 1024


def rdma(src, dst, send, recv, where):
    return pltpu.make_async_remote_copy(
        src_ref=src, dst_ref=dst, send_sem=send, recv_sem=recv,
        device_id=where, device_id_type=pl.DeviceIdType.MESH,
    )


def signal(sem, where):
    pl.semaphore_signal(sem, inc=1, device_id=where, device_id_type=pl.DeviceIdType.MESH)


def neighbours(planes, i, masks):
    v = planes[i]
    first_y, last_y, first_z, last_z = masks
    beside = planes[i + 1] + planes[i - 1]
    beside = beside + jnp.where(first_y, 0.0, pltpu.roll(v, 1, 0)) + jnp.where(last_y, 0.0, pltpu.roll(v, 15, 0))
    return beside + jnp.where(first_z, 0.0, pltpu.roll(v, 1, 1)) + jnp.where(last_z, 0.0, pltpu.roll(v, 127, 1))


def make_masks():
    rows = lax.broadcasted_iota(jnp.int32, (16, 128), 0)
    lanes = lax.broadcasted_iota(jnp.int32, (16, 128), 1)
    return rows == 0, rows == 15, lanes == 0, lanes == 127


def fields_of(w, kap, mas, inside, masks):
    sixth = 1.0 / 6.0
    diag = [6.0 - kap[i] + CENTER * mas[i] for i in range(8)]

    def op(planes, i, k):
        return diag[k] * planes[i] - neighbours(planes, i, masks)

    z00, z01, p0, p1 = [], [], [], []
    for i in range(8):
        a = op(w, i + 1, i)
        b = mas[i] * w[i + 1]
        z00.append(a)
        z01.append(b)
        p0.append((a - K0 * w[i + 1]) * (sixth * inside[i]))
        p1.append((b - w[i + 1]) * sixth)
    z10, z11, z12, q0, q1, q2 = [], [], [], [], [], []
    for i in range(6):
        k = i + 1
        a = op(p0, k, k)
        b = op(p1, k, k) + mas[k] * p0[k]
        c = mas[k] * p1[k]
        z10.append(a)
        z11.append(b)
        z12.append(c)
        q0.append((a - K0 * p0[k]) * (sixth * inside[k]))
        q1.append((b - K0 * p1[k] - p0[k]) * (sixth * inside[k]))
        q2.append((c - p1[k]) * sixth)
    z20, z21, z22, z23 = [], [], [], []
    for i in range(4):
        k, n = i + 2, i + 1
        z20.append(op(q0, n, k))
        z21.append(op(q1, n, k) + mas[k] * q0[n])
        z22.append(op(q2, n, k) + mas[k] * q1[n])
        z23.append(mas[k] * q2[n])
    zs = [w[3:7], z00[2:6], z01[2:6], z10[1:5], z11[1:5], z12[1:5], z20, z21, z22, z23]
    return zs


def inside_of(d, doms):
    out = []
    for i in range(8):
        plane = d * 4 + (i - 2)
        ok = (plane >= 0) & (plane < doms * 4)
        out.append(jnp.where(ok, 1.0, 0.0).astype(F32))
    return out


def small_solve(gram, h):
    ridge = 0.001 * (gram(1, 1) + gram(2, 2) + gram(3, 3)) / 3.0 + 1.0
    e00, e11, e22 = gram(1, 1) + ridge, gram(2, 2) + ridge, gram(3, 3) + ridge
    e10, e20, e21 = gram(2, 1), gram(3, 1), gram(3, 2)
    l00 = jnp.sqrt(e00)
    l10 = e10 / l00
    l20 = e20 / l00
    l11 = jnp.sqrt(e11 - l10 * l10)
    l21 = (e21 - l20 * l10) / l11
    l22 = jnp.sqrt(e22 - l20 * l20 - l21 * l21)
    f0 = h(1) / l00
    f1 = (h(2) - l10 * f0) / l11
    f2 = (h(3) - l20 * f0 - l21 * f1) / l22
    c2 = f2 / l22
    c1 = (f1 - l21 * c2) / l11
    c0 = (f0 - l10 * c1 - l20 * c2) / l00
    return c0, c1, c2


def powers_of(t):
    return [jnp.ones_like(t), t, t * t, t * t * t]


def by_lane(shape, dim_size, values, group):
    lane = lax.broadcasted_iota(jnp.int32, shape, 1)
    which = (lane % 32) // group
    out = jnp.zeros(shape, F32)
    for j, v in enumerate(values):
        out = jnp.where(which == j, v, out)
    return out


def main_kernel(
    doms, zs, table, ids, src, kap, mas, s_ref, fields, coef,
    buf, wide, cw, fb, gb, ob, part, r1, mine, r2, dm, dp, ds, rd, gall,
    loc, ssem, fsem, hs, hr, cs, cr, gs, gr, s1, e1, s2, e2, s3, e3, s4, e4, s5, e5,
):
    d, z = lax.axis_index("dom"), lax.axis_index("shift")
    up, down, far = lax.rem(z + 1, zs), lax.rem(z + zs - 1, zs), lax.rem(z + 2, zs)
    core, chip, chips = lax.rem(d, 2), d // 2, doms // 2
    partner = {"dom": d + 1 - 2 * core}
    has_l, has_r = d > 0, d < doms - 1
    copies = [
        pltpu.make_async_copy(src, wide.at[z, :, pl.ds(3, 4)], loc.at[0]),
        pltpu.make_async_copy(kap, cw.at[0, pl.ds(2, 4)], loc.at[1]),
        pltpu.make_async_copy(mas, cw.at[1, pl.ds(2, 4)], loc.at[2]),
    ]
    pairs = [pltpu.make_async_copy(s_ref.at[:, q], buf.at[q], ssem.at[q]) for q in range(32)]
    for c in copies + pairs:
        c.start()
    bar = pltpu.get_barrier_semaphore()
    for k in range(1, doms):
        signal(bar, {"dom": lax.rem(d + k, doms)})
    for k in range(1, zs):
        signal(bar, {"shift": lax.rem(z + k, zs)})

    @pl.when(d == 0)
    def _():
        for g in range(4):
            for s in range(8):
                wide[g, s, 0:3] = jnp.zeros((3, 16, 128), F32)
        cw[:, 0:2] = jnp.zeros((2, 2, 16, 128), F32)

    @pl.when(d == doms - 1)
    def _():
        for g in range(4):
            for s in range(8):
                wide[g, s, 7:10] = jnp.zeros((3, 16, 128), F32)
        cw[:, 6:8] = jnp.zeros((2, 2, 16, 128), F32)

    for c in copies:
        c.wait()
    pl.semaphore_wait(bar, doms + zs - 2)

    def piece(n):
        g = (z, z, down, up, far)[n]
        return g, (pl.ds(4 * n, 4) if n < 2 else pl.ds(0, 8))

    def to_left(n):
        g, s = piece(n)
        return rdma(wide.at[g, s, pl.ds(3, 3)], wide.at[g, s, pl.ds(7, 3)], hs.at[0, n], hr.at[0, n], {"dom": d - 1})

    def to_right(n):
        g, s = piece(n)
        return rdma(wide.at[g, s, pl.ds(4, 3)], wide.at[g, s, pl.ds(0, 3)], hs.at[1, n], hr.at[1, n], {"dom": d + 1})

    def coeff_left():
        return rdma(cw.at[:, pl.ds(2, 2)], cw.at[:, pl.ds(6, 2)], cs.at[0], cr.at[0], {"dom": d - 1})

    def coeff_right():
        return rdma(cw.at[:, pl.ds(4, 2)], cw.at[:, pl.ds(0, 2)], cs.at[1], cr.at[1], {"dom": d + 1})

    def start_halo(g):
        @pl.when(has_l)
        def _():
            to_left(g).start()

        @pl.when(has_r)
        def _():
            to_right(g).start()

    def wait_halo(g):
        @pl.when(has_l)
        def _():
            to_right(g).wait_recv()

        @pl.when(has_r)
        def _():
            to_left(g).wait_recv()

    @pl.when(has_l)
    def _():
        coeff_left().start()

    @pl.when(has_r)
    def _():
        coeff_right().start()

    start_halo(0)
    start_halo(1)
    own = wide.at[z, :, pl.ds(3, 4)]
    send_up = rdma(own, own, gs.at[0], gr.at[0], {"shift": up})
    send_down = rdma(own, own, gs.at[1], gr.at[1], {"shift": down})
    send_up.start()
    send_down.start()

    @pl.when(has_l)
    def _():
        coeff_right().wait_recv()

    @pl.when(has_r)
    def _():
        coeff_left().wait_recv()

    wait_halo(0)
    masks = make_masks()
    inside = inside_of(d, doms)

    def fields_for(g, sketched, begin=0, end=8):
        def one(s, carry):
            k = [cw[0, i] for i in range(8)]
            m = [cw[1, i] for i in range(8)]
            zf = fields_of([wide[g, s, i] for i in range(10)], k, m, inside, masks)
            at = g * 8 + s
            for n in range(10):
                for x in range(4):
                    fb[at, n, x] = zf[n][x]
            if sketched:
                col = pl.multiple_of(s * 16, 16)
                for x in range(4):
                    high = [zf[n][x] for n in ORDER]
                    low = [h - h.astype(BF16).astype(F32) for h in high[:LOWS]]
                    turned = jnp.transpose(jnp.stack(high + low, axis=0), (1, 0, 2)).astype(BF16)
                    for y in range(16):
                        gb[x * 8 + y // 2, pl.ds((y % 2) * 128 + col, 16), :] = turned[y]
            return carry

        lax.fori_loop(begin, end, one, 0)

    def save(g):
        return pltpu.make_async_copy(fb.at[pl.ds(g * 8, 8)], fields.at[pl.ds(g * 8, 8)], fsem.at[g])

    fields_for(z, True, 0, 4)
    wait_halo(1)
    fields_for(z, True, 4, 8)

    send_up.wait_recv()
    half_a = wide.at[down, pl.ds(0, 4), pl.ds(3, 4)]
    relay_up = rdma(half_a, half_a, gs.at[2], gr.at[2], {"shift": up})
    relay_up.start()
    send_down.wait_recv()
    half_b = wide.at[up, pl.ds(4, 4), pl.ds(3, 4)]
    relay_down = rdma(half_b, half_b, gs.at[3], gr.at[3], {"shift": down})
    relay_down.start()
    start_halo(2)
    start_halo(3)
    for c in pairs:
        c.wait()
    save(z).start()

    rows = buf.reshape(32, 2048, 128)
    even = lax.broadcasted_iota(jnp.int32, (256, 128), 0) % 2 == 0
    other = pl.multiple_of((1 - core) * 128, 128)
    keep = pl.multiple_of(core * 128, 128)

    def swap(i):
        return rdma(part.at[i, pl.ds(other, 128)], r1.at[i], s1.at[i], e1.at[i], partner)

    def scatter(i, k):
        t = lax.rem(chip + k, chips)
        return rdma(
            mine.at[i, pl.ds(pl.multiple_of(t * 8, 8), 8)], r2.at[k, i], s2.at[k, i], e2.at[k, i], {"dom": 2 * t + core}
        )

    def spread(i):
        swap(i).wait_recv()
        mine[i] = part[i, pl.ds(keep, 128)] + r1[i]
        for k in range(1, chips):
            scatter(i, k).start()

    def stage(i, carry):
        rhs = jnp.concatenate([gb[q] for q in range(32)], axis=1)
        at, bt = pl.multiple_of(i * 256, 256), pl.multiple_of(i * 256 + 1024, 256)
        lhs = jnp.concatenate(
            [jnp.concatenate([rows[q, pl.ds(at, 256), :], rows[q, pl.ds(bt, 256), :]], axis=0) for q in range(32)], axis=1
        )
        ob[...] = lax.dot_general(lhs, rhs, (((1,), (1,)), ((), ())), preferred_element_type=F32)
        a, b = ob[0:256], ob[256:512]
        xa = a[:, :128] + pltpu.roll(a[:, 128:], 255, 0)
        xb = b[:, 128:] + pltpu.roll(b[:, :128], 1, 0)
        part[i] = jnp.where(even, xa, xb)
        swap(i).start()

        @pl.when(i > 0)
        def _():
            spread(i - 1)

        return carry

    lax.fori_loop(0, 4, stage, 0)
    spread(3)
    relay_up.wait_recv()
    relay_down.wait_recv()
    start_halo(4)
    wait_halo(2)
    fields_for(down, False)

    v = []
    for i in range(4):
        total = mine[i, pl.ds(pl.multiple_of(chip * 8, 8), 8)]
        for k in range(1, chips):
            scatter(i, k).wait_recv()
            total = total + r2[k, i]
        v.append(total)
    v = jnp.concatenate(v, axis=0)
    lane = lax.broadcasted_iota(jnp.int32, (32, 128), 1) % 16
    v = v + jnp.where(lane < LOWS, pltpu.roll(v, 118, 1), 0.0)
    v = jnp.where(lane < 10, v, 0.0)
    full = lax.dot_general(v, v, (((0,), (0,)), ((), ())), precision=lax.Precision.HIGHEST, preferred_element_type=F32)
    owner = lax.broadcasted_iota(jnp.int32, (16, 128), 1) // 16
    diag = jnp.zeros((16, 128), F32)
    for s in range(8):
        diag = jnp.where(owner == s, full[16 * s : 16 * s + 16], diag)
    dm[...] = diag
    pair = rdma(dm, dp, s3, e3, partner)
    pair.start()
    save(down).start()
    pair.wait_recv()
    ds[...] = diag + dp[...]
    sums = []
    for k in range(1, chips):
        c = rdma(ds, rd.at[k], s4.at[k], e4.at[k], {"dom": 2 * lax.rem(chip + k, chips) + core})
        c.start()
        sums.append(c)
    wait_halo(3)
    fields_for(up, False)
    total = ds[...]
    for k, c in zip(range(1, chips), sums):
        c.wait_recv()
        total = total + rd[k]
    gall[z] = total
    tail = []
    for k in range(1, zs):
        c = rdma(gall.at[z], gall.at[z], s5.at[k], e5.at[k], {"shift": lax.rem(z + k, zs)})
        c.start()
        tail.append(c)
    save(up).start()
    wait_halo(4)
    fields_for(far, False)

    shifts = [table[ids[j]] - CENTER for j in range(4)]
    r = lax.broadcasted_iota(jnp.int32, (128, 128), 0)
    l = lax.broadcasted_iota(jnp.int32, (128, 128), 1)
    tw = by_lane((128, 128), 128, shifts, 8)
    pw = powers_of(tw)
    fold = jnp.zeros((128, 128), F32)
    for n in range(10):
        hit = (r % 16 == n) & (r // 16 == l % 8) & (l // 32 == OWNER[n])
        fold = jnp.where(hit, pw[DEGREE[n]], fold)
    for c in tail:
        c.wait_recv()
    mixed = lax.dot_general(
        gall[...].reshape(64, 128), fold, (((1,), (0,)), ((), ())), precision=lax.Precision.HIGHEST, preferred_element_type=F32
    )
    save(far).start()
    t = by_lane((1, 128), 128, shifts, 8)
    pt = powers_of(t)
    lines = []
    for i in range(1, 4):
        per_z = []
        for g in range(4):
            acc = jnp.zeros((1, 128), F32)
            for n in range(10):
                if OWNER[n] == i:
                    acc = acc + pt[DEGREE[n]] * mixed[g * 16 + n : g * 16 + n + 1]
            per_z.append(acc)
        lines.append(jnp.concatenate(per_z + per_z, axis=0))

    def gram(i, k):
        return lines[i - 1] if k == 0 else pltpu.roll(lines[i - 1], 128 - 32 * k, 1)

    c0, c1, c2 = small_solve(gram, lambda i: gram(i, 0))
    t = by_lane((8, 128), 128, shifts, 8)
    center = K0 + t
    sixth = 1.0 / 6.0
    e = c1 - c2 * center * sixth
    out = [c0, c0 * t, c1, c1 * t, c1 * t * t, c2, c2 * t, c2 * t * t, c2 * t * t * t]
    out += [c0 - e * center * sixth, e * sixth, e * t * sixth, c2 * sixth, c2 * t * sixth, c2 * t * t * sixth, c2]
    quarter = lax.broadcasted_iota(jnp.int32, (8, 128), 1) // 32
    for n4 in range(4):
        acc = jnp.zeros((8, 128), F32)
        for k in range(4):
            c = out[n4 * 4 + k]
            acc = jnp.where(quarter == k, c if k == 0 else pltpu.roll(c, 32 * k, 1), acc)
        coef[n4 * 8 : n4 * 8 + 8] = acc

    for i in range(4):
        swap(i).wait_send()
        for k in range(1, chips):
            scatter(i, k).wait_send()
    for c in [pair, send_up, send_down, relay_up, relay_down] + sums + tail:
        c.wait_send()

    @pl.when(has_l)
    def _():
        coeff_left().wait_send()
        for n in range(5):
            to_left(n).wait_send()

    @pl.when(has_r)
    def _():
        coeff_right().wait_send()
        for n in range(5):
            to_right(n).wait_send()

    for g in range(4):
        save(g).wait()


def output_kernel(chunks, step, coef, fields, sol, res, fin, so, ro, isem, osem):
    def take(i):
        part = pl.ds(i * step, step)
        return pltpu.make_async_copy(fields.at[part], fin.at[part], isem.at[i])

    def put(i):
        part = pl.ds(i * step, step)
        return [
            pltpu.make_async_copy(so.at[:, part], sol.at[:, part], osem.at[0, i]),
            pltpu.make_async_copy(ro.at[:, part], res.at[:, part], osem.at[1, i]),
        ]

    for i in range(chunks):
        take(i).start()

    def chunk(i, carry):
        take(i).wait()

        def one(k, carry):
            b = i * step + k
            g, s = b // 8, lax.rem(b, 8)
            for j in range(4):
                c = [coef[(n // 4) * 8 + g, (n % 4) * 32 + j * 8 + s] for n in range(15)]
                for x in range(4):
                    f = [fin[b, n, x] for n in range(10)]
                    u = c[9] * f[0]
                    for n in range(1, 6):
                        u = u + c[9 + n] * f[n]
                    r = f[0] - c[0] * f[1]
                    for n in range(1, 9):
                        r = r - c[n] * f[n + 1]
                    so[j, b, x] = u
                    ro[j, b, x] = r
            return carry

        lax.fori_loop(0, step, one, 0)

        @pl.when(i > 0)
        def _():
            for c in put(i - 1):
                c.start()

        return carry

    lax.fori_loop(0, chunks, chunk, 0)
    for c in put(chunks - 1):
        c.start()
    for i in range(chunks):
        for c in put(i):
            c.wait()


def on_device(sources, kappa, mass, shift_table, shift_ids, sketch):
    doms, zs = lax.axis_size("dom"), lax.axis_size("shift")
    sds = jax.ShapeDtypeStruct
    dma = pltpu.SemaphoreType.DMA
    smem = pl.BlockSpec(memory_space=pltpu.SMEM)
    hbm = pl.BlockSpec(memory_space=ANY)
    fields, coef = pl.pallas_call(
        functools.partial(main_kernel, doms, zs),
        out_shape=(sds((32, 10, 4, 16, 128), F32), sds((32, 128), F32)),
        in_specs=[smem, smem, hbm, hbm, hbm, hbm],
        out_specs=(hbm, pl.BlockSpec(memory_space=VMEM)),
        scratch_shapes=[
            VMEM((32, 1024, 2, 128), BF16), VMEM((4, 8, 10, 16, 128), F32), VMEM((2, 8, 16, 128), F32),
            VMEM((32, 10, 4, 16, 128), F32), VMEM((32, 256, 128), BF16), VMEM((512, 256), F32),
            VMEM((4, 256, 128), F32), VMEM((4, 128, 128), F32), VMEM((4, 128, 128), F32), VMEM((16, 4, 8, 128), F32),
            VMEM((16, 128), F32), VMEM((16, 128), F32), VMEM((16, 128), F32), VMEM((16, 16, 128), F32), VMEM((4, 16, 128), F32),
            dma((3,)), dma((32,)), dma((4,)), dma((2, 5)), dma((2, 5)), dma((2,)), dma((2,)), dma((4,)), dma((4,)),
            dma((4,)), dma((4,)), dma((16, 4)), dma((16, 4)), dma, dma, dma((16,)), dma((16,)), dma((4,)), dma((4,)),
        ],
        compiler_params=pltpu.CompilerParams(collective_id=0, has_side_effects=True, vmem_limit_bytes=56 * MiB),
        name="main",
    )(shift_table, shift_ids, sources, kappa, mass, sketch.reshape(1024, 32, 2, 128))
    step, chunks = 2, 16
    out = sds((4, 32, 4, 16, 128), F32)
    return pl.pallas_call(
        functools.partial(output_kernel, chunks, step),
        out_shape=(out, out),
        in_specs=[smem, hbm],
        out_specs=(hbm, hbm),
        scratch_shapes=[
            VMEM((32, 10, 4, 16, 128), F32), VMEM((4, 32, 4, 16, 128), F32), VMEM((4, 32, 4, 16, 128), F32),
            dma((chunks,)), dma((2, chunks)),
        ],
        compiler_params=pltpu.CompilerParams(vmem_limit_bytes=60 * MiB),
        name="outputs",
    )(coef, fields)


def solution(mesh):
    placed = (
        P("shift", "dom", None, None), P("dom", None, None), P("dom", None, None), P(), P("shift"),
        P(None, "dom", None, None),
    )
    return jax.shard_map(
        on_device,
        mesh=mesh,
        in_specs=placed,
        out_specs=(P("shift", None, "dom", None, None), P("shift", None, "dom", None, None)),
        check_vma=False,
    )
```

```python
import functools
import jax
import jax.numpy as jnp
from jax import lax
from jax.experimental import pallas as pl
from jax.experimental.pallas import tpu as pltpu
from jax.sharding import PartitionSpec as P

F32 = jnp.float32
BF16 = jnp.bfloat16
CENTER = 2.25
K0 = 6.0 + CENTER
ORDER = (0, 1, 3, 4, 6, 7, 2, 5, 8, 9)
OWNER = (0, 1, 2, 2, 3, 3, 1, 2, 3, 3)
DEGREE = (0, 0, 0, 1, 0, 1, 1, 2, 2, 3)
LOWS = 6
VMEM = pltpu.VMEM
ANY = pl.ANY
MiB = 1024 * 1024


def rdma(src, dst, send, recv, where):
    return pltpu.make_async_remote_copy(
        src_ref=src, dst_ref=dst, send_sem=send, recv_sem=recv,
        device_id=where, device_id_type=pl.DeviceIdType.MESH,
    )


def signal(sem, where):
    pl.semaphore_signal(sem, inc=1, device_id=where, device_id_type=pl.DeviceIdType.MESH)


def neighbours(planes, i, masks):
    v = planes[i]
    first_y, last_y, first_z, last_z = masks
    beside = planes[i + 1] + planes[i - 1]
    beside = beside + jnp.where(first_y, 0.0, pltpu.roll(v, 1, 0)) + jnp.where(last_y, 0.0, pltpu.roll(v, 15, 0))
    return beside + jnp.where(first_z, 0.0, pltpu.roll(v, 1, 1)) + jnp.where(last_z, 0.0, pltpu.roll(v, 127, 1))


def make_masks():
    rows = lax.broadcasted_iota(jnp.int32, (16, 128), 0)
    lanes = lax.broadcasted_iota(jnp.int32, (16, 128), 1)
    return rows == 0, rows == 15, lanes == 0, lanes == 127


def fields_of(w, kap, mas, inside, masks):
    sixth = 1.0 / 6.0
    diag = [6.0 - kap[i] + CENTER * mas[i] for i in range(8)]

    def op(planes, i, k):
        return diag[k] * planes[i] - neighbours(planes, i, masks)

    z00, z01, p0, p1 = [], [], [], []
    for i in range(8):
        a = op(w, i + 1, i)
        b = mas[i] * w[i + 1]
        z00.append(a)
        z01.append(b)
        p0.append((a - K0 * w[i + 1]) * (sixth * inside[i]))
        p1.append((b - w[i + 1]) * sixth)
    z10, z11, z12, q0, q1, q2 = [], [], [], [], [], []
    for i in range(6):
        k = i + 1
        a = op(p0, k, k)
        b = op(p1, k, k) + mas[k] * p0[k]
        c = mas[k] * p1[k]
        z10.append(a)
        z11.append(b)
        z12.append(c)
        q0.append((a - K0 * p0[k]) * (sixth * inside[k]))
        q1.append((b - K0 * p1[k] - p0[k]) * (sixth * inside[k]))
        q2.append((c - p1[k]) * sixth)
    z20, z21, z22, z23 = [], [], [], []
    for i in range(4):
        k, n = i + 2, i + 1
        z20.append(op(q0, n, k))
        z21.append(op(q1, n, k) + mas[k] * q0[n])
        z22.append(op(q2, n, k) + mas[k] * q1[n])
        z23.append(mas[k] * q2[n])
    zs = [w[3:7], z00[2:6], z01[2:6], z10[1:5], z11[1:5], z12[1:5], z20, z21, z22, z23]
    return zs


def inside_of(d, doms):
    out = []
    for i in range(8):
        plane = d * 4 + (i - 2)
        ok = (plane >= 0) & (plane < doms * 4)
        out.append(jnp.where(ok, 1.0, 0.0).astype(F32))
    return out


def small_solve(gram, h):
    ridge = 0.001 * (gram(1, 1) + gram(2, 2) + gram(3, 3)) / 3.0 + 1.0
    e00, e11, e22 = gram(1, 1) + ridge, gram(2, 2) + ridge, gram(3, 3) + ridge
    e10, e20, e21 = gram(2, 1), gram(3, 1), gram(3, 2)
    l00 = jnp.sqrt(e00)
    l10 = e10 / l00
    l20 = e20 / l00
    l11 = jnp.sqrt(e11 - l10 * l10)
    l21 = (e21 - l20 * l10) / l11
    l22 = jnp.sqrt(e22 - l20 * l20 - l21 * l21)
    f0 = h(1) / l00
    f1 = (h(2) - l10 * f0) / l11
    f2 = (h(3) - l20 * f0 - l21 * f1) / l22
    c2 = f2 / l22
    c1 = (f1 - l21 * c2) / l11
    c0 = (f0 - l10 * c1 - l20 * c2) / l00
    return c0, c1, c2


def powers_of(t):
    return [jnp.ones_like(t), t, t * t, t * t * t]


def by_lane(shape, dim_size, values, group):
    lane = lax.broadcasted_iota(jnp.int32, shape, 1)
    which = (lane % 32) // group
    out = jnp.zeros(shape, F32)
    for j, v in enumerate(values):
        out = jnp.where(which == j, v, out)
    return out


def main_kernel(
    doms, zs, table_hbm, ids_hbm, src, kap, mas, s_ref, fields, coef,
    table, ids, buf, wide, cw, fb, gb, ob, part, r1, mine, r2, dm, dp, ds, rd, gall,
    loc, ssem, fsem, hs, hr, cs, cr, gs, gr, s1, e1, s2, e2, s3, e3, s4, e4, s5, e5,
):
    d, z = lax.axis_index("dom"), lax.axis_index("shift")
    up, down, far = lax.rem(z + 1, zs), lax.rem(z + zs - 1, zs), lax.rem(z + 2, zs)
    core, chip, chips = lax.rem(d, 2), d // 2, doms // 2
    partner = {"dom": d + 1 - 2 * core}
    has_l, has_r = d > 0, d < doms - 1
    copies = [
        pltpu.make_async_copy(src, wide.at[z, :, pl.ds(3, 4)], loc.at[0]),
        pltpu.make_async_copy(kap, cw.at[0, pl.ds(2, 4)], loc.at[1]),
        pltpu.make_async_copy(mas, cw.at[1, pl.ds(2, 4)], loc.at[2]),
    ]
    tables = [
        pltpu.make_async_copy(table_hbm, table, loc.at[3]),
        pltpu.make_async_copy(ids_hbm, ids, loc.at[4]),
    ]
    pairs = [pltpu.make_async_copy(s_ref.at[:, q], buf.at[q], ssem.at[q]) for q in range(32)]
    for c in copies + tables:
        c.start()
    bar = pltpu.get_barrier_semaphore()
    for k in range(1, doms):
        signal(bar, {"dom": lax.rem(d + k, doms)})
    for k in range(1, zs):
        signal(bar, {"shift": lax.rem(z + k, zs)})

    @pl.when(d == 0)
    def _():
        for g in range(4):
            for s in range(8):
                wide[g, s, 0:3] = jnp.zeros((3, 16, 128), F32)
        cw[:, 0:2] = jnp.zeros((2, 2, 16, 128), F32)

    @pl.when(d == doms - 1)
    def _():
        for g in range(4):
            for s in range(8):
                wide[g, s, 7:10] = jnp.zeros((3, 16, 128), F32)
        cw[:, 6:8] = jnp.zeros((2, 2, 16, 128), F32)

    for c in copies:
        c.wait()
    pl.semaphore_wait(bar, doms + zs - 2)

    def piece(n):
        g = (z, z, down, up, far)[n]
        return g, (pl.ds(4 * n, 4) if n < 2 else pl.ds(0, 8))

    def to_left(n):
        g, s = piece(n)
        return rdma(wide.at[g, s, pl.ds(3, 3)], wide.at[g, s, pl.ds(7, 3)], hs.at[0, n], hr.at[0, n], {"dom": d - 1})

    def to_right(n):
        g, s = piece(n)
        return rdma(wide.at[g, s, pl.ds(4, 3)], wide.at[g, s, pl.ds(0, 3)], hs.at[1, n], hr.at[1, n], {"dom": d + 1})

    def coeff_left():
        return rdma(cw.at[:, pl.ds(2, 2)], cw.at[:, pl.ds(6, 2)], cs.at[0], cr.at[0], {"dom": d - 1})

    def coeff_right():
        return rdma(cw.at[:, pl.ds(4, 2)], cw.at[:, pl.ds(0, 2)], cs.at[1], cr.at[1], {"dom": d + 1})

    def start_halo(g):
        @pl.when(has_l)
        def _():
            to_left(g).start()

        @pl.when(has_r)
        def _():
            to_right(g).start()

    def wait_halo(g):
        @pl.when(has_l)
        def _():
            to_right(g).wait_recv()

        @pl.when(has_r)
        def _():
            to_left(g).wait_recv()

    @pl.when(has_l)
    def _():
        coeff_left().start()

    @pl.when(has_r)
    def _():
        coeff_right().start()

    start_halo(0)
    start_halo(1)
    own = wide.at[z, :, pl.ds(3, 4)]
    for c in pairs:
        c.start()
    send_up = rdma(own, own, gs.at[0], gr.at[0], {"shift": up})
    send_down = rdma(own, own, gs.at[1], gr.at[1], {"shift": down})
    send_up.start()
    send_down.start()

    @pl.when(has_l)
    def _():
        coeff_right().wait_recv()

    @pl.when(has_r)
    def _():
        coeff_left().wait_recv()

    wait_halo(0)
    masks = make_masks()
    inside = inside_of(d, doms)

    def fields_for(g, sketched, begin=0, end=8):
        def one(s, carry):
            k = [cw[0, i] for i in range(8)]
            m = [cw[1, i] for i in range(8)]
            zf = fields_of([wide[g, s, i] for i in range(10)], k, m, inside, masks)
            at = g * 8 + s
            for n in range(10):
                for x in range(4):
                    fb[at, n, x] = zf[n][x]
            if sketched:
                col = pl.multiple_of(s * 16, 16)
                for x in range(4):
                    high = [zf[n][x] for n in ORDER]
                    low = [h - h.astype(BF16).astype(F32) for h in high[:LOWS]]
                    turned = jnp.transpose(jnp.stack(high + low, axis=0), (1, 0, 2)).astype(BF16)
                    for y in range(16):
                        gb[x * 8 + y // 2, pl.ds((y % 2) * 128 + col, 16), :] = turned[y]
            return carry

        lax.fori_loop(begin, end, one, 0)

    def save(g):
        return pltpu.make_async_copy(fb.at[pl.ds(g * 8, 8)], fields.at[pl.ds(g * 8, 8)], fsem.at[g])

    fields_for(z, True, 0, 4)
    wait_halo(1)
    fields_for(z, True, 4, 8)

    send_up.wait_recv()
    half_a = wide.at[down, pl.ds(0, 4), pl.ds(3, 4)]
    relay_up = rdma(half_a, half_a, gs.at[2], gr.at[2], {"shift": up})
    relay_up.start()
    send_down.wait_recv()
    half_b = wide.at[up, pl.ds(4, 4), pl.ds(3, 4)]
    relay_down = rdma(half_b, half_b, gs.at[3], gr.at[3], {"shift": down})
    relay_down.start()
    start_halo(2)
    start_halo(3)
    for c in tables + pairs:
        c.wait()
    save(z).start()

    rows = buf.reshape(32, 2048, 128)
    even = lax.broadcasted_iota(jnp.int32, (256, 128), 0) % 2 == 0
    other = pl.multiple_of((1 - core) * 128, 128)
    keep = pl.multiple_of(core * 128, 128)

    def swap(i):
        return rdma(part.at[i, pl.ds(other, 128)], r1.at[i], s1.at[i], e1.at[i], partner)

    def scatter(i, k):
        t = lax.rem(chip + k, chips)
        return rdma(
            mine.at[i, pl.ds(pl.multiple_of(t * 8, 8), 8)], r2.at[k, i], s2.at[k, i], e2.at[k, i], {"dom": 2 * t + core}
        )

    def spread(i):
        swap(i).wait_recv()
        mine[i] = part[i, pl.ds(keep, 128)] + r1[i]
        for k in range(1, chips):
            scatter(i, k).start()

    def stage(i, carry):
        rhs = jnp.concatenate([gb[q] for q in range(32)], axis=1)
        at, bt = pl.multiple_of(i * 256, 256), pl.multiple_of(i * 256 + 1024, 256)
        lhs = jnp.concatenate(
            [jnp.concatenate([rows[q, pl.ds(at, 256), :], rows[q, pl.ds(bt, 256), :]], axis=0) for q in range(32)], axis=1
        )
        ob[...] = lax.dot_general(lhs, rhs, (((1,), (1,)), ((), ())), preferred_element_type=F32)
        a, b = ob[0:256], ob[256:512]
        xa = a[:, :128] + pltpu.roll(a[:, 128:], 255, 0)
        xb = b[:, 128:] + pltpu.roll(b[:, :128], 1, 0)
        part[i] = jnp.where(even, xa, xb)
        swap(i).start()

        @pl.when(i > 0)
        def _():
            spread(i - 1)

        return carry

    lax.fori_loop(0, 4, stage, 0)
    spread(3)
    relay_up.wait_recv()
    relay_down.wait_recv()
    start_halo(4)
    wait_halo(2)
    fields_for(down, False)

    v = []
    for i in range(4):
        total = mine[i, pl.ds(pl.multiple_of(chip * 8, 8), 8)]
        for k in range(1, chips):
            scatter(i, k).wait_recv()
            total = total + r2[k, i]
        v.append(total)
    v = jnp.concatenate(v, axis=0)
    lane = lax.broadcasted_iota(jnp.int32, (32, 128), 1) % 16
    v = v + jnp.where(lane < LOWS, pltpu.roll(v, 118, 1), 0.0)
    v = jnp.where(lane < 10, v, 0.0)
    full = lax.dot_general(v, v, (((0,), (0,)), ((), ())), precision=lax.Precision.HIGHEST, preferred_element_type=F32)
    owner = lax.broadcasted_iota(jnp.int32, (16, 128), 1) // 16
    diag = jnp.zeros((16, 128), F32)
    for s in range(8):
        diag = jnp.where(owner == s, full[16 * s : 16 * s + 16], diag)
    dm[...] = diag
    pair = rdma(dm, dp, s3, e3, partner)
    pair.start()
    save(down).start()
    pair.wait_recv()
    ds[...] = diag + dp[...]
    sums = []
    for k in range(1, chips):
        c = rdma(ds, rd.at[k], s4.at[k], e4.at[k], {"dom": 2 * lax.rem(chip + k, chips) + core})
        c.start()
        sums.append(c)
    wait_halo(3)
    fields_for(up, False)
    total = ds[...]
    for k, c in zip(range(1, chips), sums):
        c.wait_recv()
        total = total + rd[k]
    gall[z] = total
    tail = []
    for k in range(1, zs):
        c = rdma(gall.at[z], gall.at[z], s5.at[k], e5.at[k], {"shift": lax.rem(z + k, zs)})
        c.start()
        tail.append(c)
    save(up).start()
    wait_halo(4)
    fields_for(far, False)

    shifts = [table[ids[j]] - CENTER for j in range(4)]
    r = lax.broadcasted_iota(jnp.int32, (128, 128), 0)
    l = lax.broadcasted_iota(jnp.int32, (128, 128), 1)
    tw = by_lane((128, 128), 128, shifts, 8)
    pw = powers_of(tw)
    fold = jnp.zeros((128, 128), F32)
    for n in range(10):
        hit = (r % 16 == n) & (r // 16 == l % 8) & (l // 32 == OWNER[n])
        fold = jnp.where(hit, pw[DEGREE[n]], fold)
    for c in tail:
        c.wait_recv()
    mixed = lax.dot_general(
        gall[...].reshape(64, 128), fold, (((1,), (0,)), ((), ())), precision=lax.Precision.HIGHEST, preferred_element_type=F32
    )
    save(far).start()
    t = by_lane((1, 128), 128, shifts, 8)
    pt = powers_of(t)
    lines = []
    for i in range(1, 4):
        per_z = []
        for g in range(4):
            acc = jnp.zeros((1, 128), F32)
            for n in range(10):
                if OWNER[n] == i:
                    acc = acc + pt[DEGREE[n]] * mixed[g * 16 + n : g * 16 + n + 1]
            per_z.append(acc)
        lines.append(jnp.concatenate(per_z + per_z, axis=0))

    def gram(i, k):
        return lines[i - 1] if k == 0 else pltpu.roll(lines[i - 1], 128 - 32 * k, 1)

    c0, c1, c2 = small_solve(gram, lambda i: gram(i, 0))
    t = by_lane((8, 128), 128, shifts, 8)
    center = K0 + t
    sixth = 1.0 / 6.0
    e = c1 - c2 * center * sixth
    out = [c0, c0 * t, c1, c1 * t, c1 * t * t, c2, c2 * t, c2 * t * t, c2 * t * t * t]
    out += [c0 - e * center * sixth, e * sixth, e * t * sixth, c2 * sixth, c2 * t * sixth, c2 * t * t * sixth, c2]
    quarter = lax.broadcasted_iota(jnp.int32, (8, 128), 1) // 32
    for n4 in range(4):
        acc = jnp.zeros((8, 128), F32)
        for k in range(4):
            c = out[n4 * 4 + k]
            acc = jnp.where(quarter == k, c if k == 0 else pltpu.roll(c, 32 * k, 1), acc)
        coef[n4 * 8 : n4 * 8 + 8] = acc

    for i in range(4):
        swap(i).wait_send()
        for k in range(1, chips):
            scatter(i, k).wait_send()
    for c in [pair, send_up, send_down, relay_up, relay_down] + sums + tail:
        c.wait_send()

    @pl.when(has_l)
    def _():
        coeff_left().wait_send()
        for n in range(5):
            to_left(n).wait_send()

    @pl.when(has_r)
    def _():
        coeff_right().wait_send()
        for n in range(5):
            to_right(n).wait_send()

    for g in range(4):
        save(g).wait()


def output_kernel(chunks, step, coef, fields, sol, res, fin, so, ro, isem, osem):
    def take(i):
        part = pl.ds(i * step, step)
        return pltpu.make_async_copy(fields.at[part], fin.at[part], isem.at[i])

    def put(i):
        part = pl.ds(i * step, step)
        return [
            pltpu.make_async_copy(so.at[:, part], sol.at[:, part], osem.at[0, i]),
            pltpu.make_async_copy(ro.at[:, part], res.at[:, part], osem.at[1, i]),
        ]

    for i in range(chunks):
        take(i).start()

    def chunk(i, carry):
        take(i).wait()

        def one(k, carry):
            b = i * step + k
            g, s = b // 8, lax.rem(b, 8)
            for j in range(4):
                c = [coef[(n // 4) * 8 + g, (n % 4) * 32 + j * 8 + s] for n in range(15)]
                for x in range(4):
                    f = [fin[b, n, x] for n in range(10)]
                    u = c[9] * f[0]
                    for n in range(1, 6):
                        u = u + c[9 + n] * f[n]
                    r = f[0] - c[0] * f[1]
                    for n in range(1, 9):
                        r = r - c[n] * f[n + 1]
                    so[j, b, x] = u
                    ro[j, b, x] = r
            return carry

        lax.fori_loop(0, step, one, 0)

        @pl.when(i > 0)
        def _():
            for c in put(i - 1):
                c.start()

        return carry

    lax.fori_loop(0, chunks, chunk, 0)
    for c in put(chunks - 1):
        c.start()
    for i in range(chunks):
        for c in put(i):
            c.wait()


def on_device(sources, kappa, mass, shift_table, shift_ids, sketch):
    doms, zs = lax.axis_size("dom"), lax.axis_size("shift")
    sds = jax.ShapeDtypeStruct
    dma = pltpu.SemaphoreType.DMA
    smem = pl.BlockSpec(memory_space=pltpu.SMEM)
    hbm = pl.BlockSpec(memory_space=ANY)
    fields, coef = pl.pallas_call(
        functools.partial(main_kernel, doms, zs),
        out_shape=(sds((32, 10, 4, 16, 128), F32), sds((32, 128), F32)),
        in_specs=[hbm] * 6,
        out_specs=(hbm, pl.BlockSpec(memory_space=VMEM)),
        scratch_shapes=[
            pltpu.SMEM((64,), F32), pltpu.SMEM((4,), jnp.int32), VMEM((32, 1024, 2, 128), BF16), VMEM((4, 8, 10, 16, 128), F32), VMEM((2, 8, 16, 128), F32),
            VMEM((32, 10, 4, 16, 128), F32), VMEM((32, 256, 128), BF16), VMEM((512, 256), F32),
            VMEM((4, 256, 128), F32), VMEM((4, 128, 128), F32), VMEM((4, 128, 128), F32), VMEM((16, 4, 8, 128), F32),
            VMEM((16, 128), F32), VMEM((16, 128), F32), VMEM((16, 128), F32), VMEM((16, 16, 128), F32), VMEM((4, 16, 128), F32),
            dma((5,)), dma((32,)), dma((4,)), dma((2, 5)), dma((2, 5)), dma((2,)), dma((2,)), dma((4,)), dma((4,)),
            dma((4,)), dma((4,)), dma((16, 4)), dma((16, 4)), dma, dma, dma((16,)), dma((16,)), dma((4,)), dma((4,)),
        ],
        compiler_params=pltpu.CompilerParams(collective_id=0, has_side_effects=True, vmem_limit_bytes=56 * MiB),
        name="main",
    )(shift_table, shift_ids, sources, kappa, mass, sketch.reshape(1024, 32, 2, 128))
    step, chunks = 2, 16
    out = sds((4, 32, 4, 16, 128), F32)
    return pl.pallas_call(
        functools.partial(output_kernel, chunks, step),
        out_shape=(out, out),
        in_specs=[smem, hbm],
        out_specs=(hbm, hbm),
        scratch_shapes=[
            VMEM((32, 10, 4, 16, 128), F32), VMEM((4, 32, 4, 16, 128), F32), VMEM((4, 32, 4, 16, 128), F32),
            dma((chunks,)), dma((2, chunks)),
        ],
        compiler_params=pltpu.CompilerParams(vmem_limit_bytes=60 * MiB),
        name="outputs",
    )(coef, fields)


def solution(mesh):
    placed = (
        P("shift", "dom", None, None), P("dom", None, None), P("dom", None, None), P(), P("shift"),
        P(None, "dom", None, None),
    )
    return jax.shard_map(
        on_device,
        mesh=mesh,
        in_specs=placed,
        out_specs=(P("shift", None, "dom", None, None), P("shift", None, "dom", None, None)),
        check_vma=False,
    )
```

```python
import functools
import jax
import jax.numpy as jnp
from jax import lax
from jax.experimental import pallas as pl
from jax.experimental.pallas import tpu as pltpu
from jax.sharding import PartitionSpec as P

F32 = jnp.float32
BF16 = jnp.bfloat16
CENTER = 2.25
K0 = 6.0 + CENTER
ORDER = (0, 1, 3, 4, 6, 7, 2, 5, 8, 9)
OWNER = (0, 1, 2, 2, 3, 3, 1, 2, 3, 3)
DEGREE = (0, 0, 0, 1, 0, 1, 1, 2, 2, 3)
LOWS = 6
VMEM = pltpu.VMEM
ANY = pl.ANY
MiB = 1024 * 1024


def rdma(src, dst, send, recv, where):
    return pltpu.make_async_remote_copy(
        src_ref=src, dst_ref=dst, send_sem=send, recv_sem=recv,
        device_id=where, device_id_type=pl.DeviceIdType.MESH,
    )


def signal(sem, where):
    pl.semaphore_signal(sem, inc=1, device_id=where, device_id_type=pl.DeviceIdType.MESH)


def neighbours(planes, i, masks):
    v = planes[i]
    first_y, last_y, first_z, last_z = masks
    beside = planes[i + 1] + planes[i - 1]
    beside = beside + jnp.where(first_y, 0.0, pltpu.roll(v, 1, 0)) + jnp.where(last_y, 0.0, pltpu.roll(v, 15, 0))
    return beside + jnp.where(first_z, 0.0, pltpu.roll(v, 1, 1)) + jnp.where(last_z, 0.0, pltpu.roll(v, 127, 1))


def make_masks():
    rows = lax.broadcasted_iota(jnp.int32, (16, 128), 0)
    lanes = lax.broadcasted_iota(jnp.int32, (16, 128), 1)
    return rows == 0, rows == 15, lanes == 0, lanes == 127


def fields_of(w, kap, mas, inside, masks):
    sixth = 1.0 / 6.0
    diag = [6.0 - kap[i] + CENTER * mas[i] for i in range(8)]

    def op(planes, i, k):
        return diag[k] * planes[i] - neighbours(planes, i, masks)

    z00, z01, p0, p1 = [], [], [], []
    for i in range(8):
        a = op(w, i + 1, i)
        b = mas[i] * w[i + 1]
        z00.append(a)
        z01.append(b)
        p0.append((a - K0 * w[i + 1]) * (sixth * inside[i]))
        p1.append((b - w[i + 1]) * sixth)
    z10, z11, z12, q0, q1, q2 = [], [], [], [], [], []
    for i in range(6):
        k = i + 1
        a = op(p0, k, k)
        b = op(p1, k, k) + mas[k] * p0[k]
        c = mas[k] * p1[k]
        z10.append(a)
        z11.append(b)
        z12.append(c)
        q0.append((a - K0 * p0[k]) * (sixth * inside[k]))
        q1.append((b - K0 * p1[k] - p0[k]) * (sixth * inside[k]))
        q2.append((c - p1[k]) * sixth)
    z20, z21, z22, z23 = [], [], [], []
    for i in range(4):
        k, n = i + 2, i + 1
        z20.append(op(q0, n, k))
        z21.append(op(q1, n, k) + mas[k] * q0[n])
        z22.append(op(q2, n, k) + mas[k] * q1[n])
        z23.append(mas[k] * q2[n])
    zs = [w[3:7], z00[2:6], z01[2:6], z10[1:5], z11[1:5], z12[1:5], z20, z21, z22, z23]
    return zs


def inside_of(d, doms):
    out = []
    for i in range(8):
        plane = d * 4 + (i - 2)
        ok = (plane >= 0) & (plane < doms * 4)
        out.append(jnp.where(ok, 1.0, 0.0).astype(F32))
    return out


def small_solve(gram, h):
    ridge = 0.001 * (gram(1, 1) + gram(2, 2) + gram(3, 3)) / 3.0 + 1.0
    e00, e11, e22 = gram(1, 1) + ridge, gram(2, 2) + ridge, gram(3, 3) + ridge
    e10, e20, e21 = gram(2, 1), gram(3, 1), gram(3, 2)
    l00 = jnp.sqrt(e00)
    l10 = e10 / l00
    l20 = e20 / l00
    l11 = jnp.sqrt(e11 - l10 * l10)
    l21 = (e21 - l20 * l10) / l11
    l22 = jnp.sqrt(e22 - l20 * l20 - l21 * l21)
    f0 = h(1) / l00
    f1 = (h(2) - l10 * f0) / l11
    f2 = (h(3) - l20 * f0 - l21 * f1) / l22
    c2 = f2 / l22
    c1 = (f1 - l21 * c2) / l11
    c0 = (f0 - l10 * c1 - l20 * c2) / l00
    return c0, c1, c2


def powers_of(t):
    return [jnp.ones_like(t), t, t * t, t * t * t]


def by_lane(shape, dim_size, values, group):
    lane = lax.broadcasted_iota(jnp.int32, shape, 1)
    which = (lane % 32) // group
    out = jnp.zeros(shape, F32)
    for j, v in enumerate(values):
        out = jnp.where(which == j, v, out)
    return out


def main_kernel(
    doms, zs, table_hbm, ids_hbm, src, kap, mas, s_ref, fields, coef,
    table, ids, buf, wide, cw, fb, gb, ob, part, r1, mine, r2, dm, dp, ds, rd, gall,
    loc, ssem, fsem, hs, hr, cs, cr, gs, gr, s1, e1, s2, e2, s3, e3, s4, e4, s5, e5,
):
    d, z = lax.axis_index("dom"), lax.axis_index("shift")
    up, down, far = lax.rem(z + 1, zs), lax.rem(z + zs - 1, zs), lax.rem(z + 2, zs)
    core, chip, chips = lax.rem(d, 2), d // 2, doms // 2
    partner = {"dom": d + 1 - 2 * core}
    has_l, has_r = d > 0, d < doms - 1
    copies = [
        pltpu.make_async_copy(src, wide.at[z, :, pl.ds(3, 4)], loc.at[0]),
        pltpu.make_async_copy(kap, cw.at[0, pl.ds(2, 4)], loc.at[1]),
        pltpu.make_async_copy(mas, cw.at[1, pl.ds(2, 4)], loc.at[2]),
    ]
    tables = [
        pltpu.make_async_copy(table_hbm, table, loc.at[3]),
        pltpu.make_async_copy(ids_hbm, ids, loc.at[4]),
    ]
    pairs = [pltpu.make_async_copy(s_ref.at[:, q], buf.at[q], ssem.at[q]) for q in range(32)]
    for c in copies + tables:
        c.start()
    bar = pltpu.get_barrier_semaphore()
    for k in range(1, doms):
        signal(bar, {"dom": lax.rem(d + k, doms)})
    for k in range(1, zs):
        signal(bar, {"shift": lax.rem(z + k, zs)})

    @pl.when(d == 0)
    def _():
        for g in range(4):
            for s in range(8):
                wide[g, s, 0:3] = jnp.zeros((3, 16, 128), F32)
        cw[:, 0:2] = jnp.zeros((2, 2, 16, 128), F32)

    @pl.when(d == doms - 1)
    def _():
        for g in range(4):
            for s in range(8):
                wide[g, s, 7:10] = jnp.zeros((3, 16, 128), F32)
        cw[:, 6:8] = jnp.zeros((2, 2, 16, 128), F32)

    for c in copies:
        c.wait()
    pl.semaphore_wait(bar, doms + zs - 2)

    def piece(n):
        g = (z, z, down, up, far)[n]
        return g, (pl.ds(4 * n, 4) if n < 2 else pl.ds(0, 8))

    def to_left(n):
        g, s = piece(n)
        return rdma(wide.at[g, s, pl.ds(3, 3)], wide.at[g, s, pl.ds(7, 3)], hs.at[0, n], hr.at[0, n], {"dom": d - 1})

    def to_right(n):
        g, s = piece(n)
        return rdma(wide.at[g, s, pl.ds(4, 3)], wide.at[g, s, pl.ds(0, 3)], hs.at[1, n], hr.at[1, n], {"dom": d + 1})

    def coeff_left():
        return rdma(cw.at[:, pl.ds(2, 2)], cw.at[:, pl.ds(6, 2)], cs.at[0], cr.at[0], {"dom": d - 1})

    def coeff_right():
        return rdma(cw.at[:, pl.ds(4, 2)], cw.at[:, pl.ds(0, 2)], cs.at[1], cr.at[1], {"dom": d + 1})

    def start_halo(g):
        @pl.when(has_l)
        def _():
            to_left(g).start()

        @pl.when(has_r)
        def _():
            to_right(g).start()

    def wait_halo(g):
        @pl.when(has_l)
        def _():
            to_right(g).wait_recv()

        @pl.when(has_r)
        def _():
            to_left(g).wait_recv()

    @pl.when(has_l)
    def _():
        coeff_left().start()

    @pl.when(has_r)
    def _():
        coeff_right().start()

    start_halo(0)
    start_halo(1)
    own = wide.at[z, :, pl.ds(3, 4)]
    for c in pairs:
        c.start()
    send_up = rdma(own, own, gs.at[0], gr.at[0], {"shift": up})
    send_down = rdma(own, own, gs.at[1], gr.at[1], {"shift": down})
    send_up.start()
    send_down.start()

    @pl.when(has_l)
    def _():
        coeff_right().wait_recv()

    @pl.when(has_r)
    def _():
        coeff_left().wait_recv()

    wait_halo(0)
    masks = make_masks()
    inside = inside_of(d, doms)

    def fields_for(g, sketched, begin=0, end=8):
        def one(s, carry):
            k = [cw[0, i] for i in range(8)]
            m = [cw[1, i] for i in range(8)]
            zf = fields_of([wide[g, s, i] for i in range(10)], k, m, inside, masks)
            at = g * 8 + s
            for n in range(10):
                for x in range(4):
                    fb[at, n, x] = zf[n][x]
            if sketched:
                col = pl.multiple_of(s * 16, 16)
                for x in range(4):
                    high = [zf[n][x] for n in ORDER]
                    low = [h - h.astype(BF16).astype(F32) for h in high[:LOWS]]
                    turned = jnp.transpose(jnp.stack(high + low, axis=0), (1, 0, 2)).astype(BF16)
                    for y in range(16):
                        gb[x * 8 + y // 2, pl.ds((y % 2) * 128 + col, 16), :] = turned[y]
            return carry

        lax.fori_loop(begin, end, one, 0)

    def save(g):
        return pltpu.make_async_copy(fb.at[pl.ds(g * 8, 8)], fields.at[pl.ds(g * 8, 8)], fsem.at[g])

    fields_for(z, True, 0, 4)
    wait_halo(1)
    fields_for(z, True, 4, 8)

    send_up.wait_recv()
    half_a = wide.at[down, pl.ds(0, 4), pl.ds(3, 4)]
    relay_up = rdma(half_a, half_a, gs.at[2], gr.at[2], {"shift": up})
    relay_up.start()
    send_down.wait_recv()
    half_b = wide.at[up, pl.ds(4, 4), pl.ds(3, 4)]
    relay_down = rdma(half_b, half_b, gs.at[3], gr.at[3], {"shift": down})
    relay_down.start()
    start_halo(2)
    start_halo(3)
    for c in tables + pairs:
        c.wait()
    save(z).start()

    rows = buf.reshape(32, 2048, 128)
    even = lax.broadcasted_iota(jnp.int32, (256, 128), 0) % 2 == 0
    other = pl.multiple_of((1 - core) * 128, 128)
    keep = pl.multiple_of(core * 128, 128)

    def swap(i):
        return rdma(part.at[i, pl.ds(other, 128)], r1.at[i], s1.at[i], e1.at[i], partner)

    def scatter(i, k):
        t = lax.rem(chip + k, chips)
        return rdma(
            mine.at[i, pl.ds(pl.multiple_of(t * 8, 8), 8)], r2.at[k, i], s2.at[k, i], e2.at[k, i], {"dom": 2 * t + core}
        )

    def spread(i):
        swap(i).wait_recv()
        mine[i] = part[i, pl.ds(keep, 128)] + r1[i]
        for k in range(1, chips):
            scatter(i, k).start()

    def stage(i, carry):
        rhs = jnp.concatenate([gb[q] for q in range(32)], axis=1)
        at, bt = pl.multiple_of(i * 256, 256), pl.multiple_of(i * 256 + 1024, 256)
        lhs = jnp.concatenate(
            [jnp.concatenate([rows[q, pl.ds(at, 256), :], rows[q, pl.ds(bt, 256), :]], axis=0) for q in range(32)], axis=1
        )
        ob[...] = lax.dot_general(lhs, rhs, (((1,), (1,)), ((), ())), preferred_element_type=F32)
        a, b = ob[0:256], ob[256:512]
        xa = a[:, :128] + pltpu.roll(a[:, 128:], 255, 0)
        xb = b[:, 128:] + pltpu.roll(b[:, :128], 1, 0)
        part[i] = jnp.where(even, xa, xb)
        swap(i).start()

        @pl.when(i > 0)
        def _():
            spread(i - 1)

        return carry

    lax.fori_loop(0, 4, stage, 0)
    spread(3)
    relay_up.wait_recv()
    relay_down.wait_recv()
    start_halo(4)
    wait_halo(2)
    fields_for(down, False)

    v = []
    for i in range(4):
        total = mine[i, pl.ds(pl.multiple_of(chip * 8, 8), 8)]
        for k in range(1, chips):
            scatter(i, k).wait_recv()
            total = total + r2[k, i]
        v.append(total)
    v = jnp.concatenate(v, axis=0)
    lane = lax.broadcasted_iota(jnp.int32, (32, 128), 1) % 16
    v = v + jnp.where(lane < LOWS, pltpu.roll(v, 118, 1), 0.0)
    v = jnp.where(lane < 10, v, 0.0)
    full = lax.dot_general(v, v, (((0,), (0,)), ((), ())), precision=lax.Precision.HIGHEST, preferred_element_type=F32)
    owner = lax.broadcasted_iota(jnp.int32, (16, 128), 1) // 16
    diag = jnp.zeros((16, 128), F32)
    for s in range(8):
        diag = jnp.where(owner == s, full[16 * s : 16 * s + 16], diag)
    dm[...] = diag
    pair = rdma(dm, dp, s3, e3, partner)
    pair.start()
    save(down).start()
    pair.wait_recv()
    ds[...] = diag + dp[...]
    sums = []
    for k in range(1, chips):
        c = rdma(ds, rd.at[k], s4.at[k], e4.at[k], {"dom": 2 * lax.rem(chip + k, chips) + core})
        c.start()
        sums.append(c)
    wait_halo(3)
    fields_for(up, False)
    total = ds[...]
    for k, c in zip(range(1, chips), sums):
        c.wait_recv()
        total = total + rd[k]
    gall[z] = total
    tail = []
    for k in range(1, zs):
        c = rdma(gall.at[z], gall.at[z], s5.at[k], e5.at[k], {"shift": lax.rem(z + k, zs)})
        c.start()
        tail.append(c)
    save(up).start()
    wait_halo(4)
    fields_for(far, False)
    save(far).start()

    shifts = [table[ids[j]] - CENTER for j in range(4)]
    r = lax.broadcasted_iota(jnp.int32, (128, 128), 0)
    l = lax.broadcasted_iota(jnp.int32, (128, 128), 1)
    tw = by_lane((128, 128), 128, shifts, 8)
    pw = powers_of(tw)
    fold = jnp.zeros((128, 128), F32)
    for n in range(10):
        hit = (r % 16 == n) & (r // 16 == l % 8) & (l // 32 == OWNER[n])
        fold = jnp.where(hit, pw[DEGREE[n]], fold)
    for c in tail:
        c.wait_recv()
    mixed = lax.dot_general(
        gall[...].reshape(64, 128), fold, (((1,), (0,)), ((), ())), precision=lax.Precision.HIGHEST, preferred_element_type=F32
    )
    t = by_lane((1, 128), 128, shifts, 8)
    pt = powers_of(t)
    lines = []
    for i in range(1, 4):
        per_z = []
        for g in range(4):
            acc = jnp.zeros((1, 128), F32)
            for n in range(10):
                if OWNER[n] == i:
                    acc = acc + pt[DEGREE[n]] * mixed[g * 16 + n : g * 16 + n + 1]
            per_z.append(acc)
        lines.append(jnp.concatenate(per_z + per_z, axis=0))

    def gram(i, k):
        return lines[i - 1] if k == 0 else pltpu.roll(lines[i - 1], 128 - 32 * k, 1)

    c0, c1, c2 = small_solve(gram, lambda i: gram(i, 0))
    t = by_lane((8, 128), 128, shifts, 8)
    center = K0 + t
    sixth = 1.0 / 6.0
    e = c1 - c2 * center * sixth
    out = [c0, c0 * t, c1, c1 * t, c1 * t * t, c2, c2 * t, c2 * t * t, c2 * t * t * t]
    out += [c0 - e * center * sixth, e * sixth, e * t * sixth, c2 * sixth, c2 * t * sixth, c2 * t * t * sixth, c2]
    quarter = lax.broadcasted_iota(jnp.int32, (8, 128), 1) // 32
    for n4 in range(4):
        acc = jnp.zeros((8, 128), F32)
        for k in range(4):
            c = out[n4 * 4 + k]
            acc = jnp.where(quarter == k, c if k == 0 else pltpu.roll(c, 32 * k, 1), acc)
        coef[n4 * 8 : n4 * 8 + 8] = acc

    for i in range(4):
        swap(i).wait_send()
        for k in range(1, chips):
            scatter(i, k).wait_send()
    for c in [pair, send_up, send_down, relay_up, relay_down] + sums + tail:
        c.wait_send()

    @pl.when(has_l)
    def _():
        coeff_left().wait_send()
        for n in range(5):
            to_left(n).wait_send()

    @pl.when(has_r)
    def _():
        coeff_right().wait_send()
        for n in range(5):
            to_right(n).wait_send()

    for g in range(4):
        save(g).wait()


def output_kernel(chunks, step, coef_hbm, fields, sol, res, coef, fin, so, ro, isem, osem, csem):
    def take(i):
        part = pl.ds(i * step, step)
        return pltpu.make_async_copy(fields.at[part], fin.at[part], isem.at[i])

    def put(i):
        part = pl.ds(i * step, step)
        return [
            pltpu.make_async_copy(so.at[:, part], sol.at[:, part], osem.at[0, i]),
            pltpu.make_async_copy(ro.at[:, part], res.at[:, part], osem.at[1, i]),
        ]

    ahead = 4
    first = pltpu.make_async_copy(coef_hbm, coef, csem)
    first.start()
    for i in range(ahead):
        take(i).start()
    first.wait()

    def chunk(i, carry):
        take(i).wait()

        @pl.when(i + ahead < chunks)
        def _():
            take(i + ahead).start()

        def one(k, carry):
            b = i * step + k
            g, s = b // 8, lax.rem(b, 8)
            for j in range(4):
                c = [coef[(n // 4) * 8 + g, (n % 4) * 32 + j * 8 + s] for n in range(15)]
                for x in range(4):
                    f = [fin[b, n, x] for n in range(10)]
                    u = c[9] * f[0]
                    for n in range(1, 6):
                        u = u + c[9 + n] * f[n]
                    r = f[0] - c[0] * f[1]
                    for n in range(1, 9):
                        r = r - c[n] * f[n + 1]
                    so[j, b, x] = u
                    ro[j, b, x] = r
            return carry

        lax.fori_loop(0, step, one, 0)

        @pl.when(i > 0)
        def _():
            for c in put(i - 1):
                c.start()

        return carry

    lax.fori_loop(0, chunks, chunk, 0)
    for c in put(chunks - 1):
        c.start()
    for i in range(chunks):
        for c in put(i):
            c.wait()


def on_device(sources, kappa, mass, shift_table, shift_ids, sketch):
    doms, zs = lax.axis_size("dom"), lax.axis_size("shift")
    sds = jax.ShapeDtypeStruct
    dma = pltpu.SemaphoreType.DMA
    hbm = pl.BlockSpec(memory_space=ANY)
    fields, coef = pl.pallas_call(
        functools.partial(main_kernel, doms, zs),
        out_shape=(sds((32, 10, 4, 16, 128), F32), sds((32, 128), F32)),
        in_specs=[hbm] * 6,
        out_specs=(hbm, pl.BlockSpec(memory_space=VMEM)),
        scratch_shapes=[
            pltpu.SMEM((64,), F32), pltpu.SMEM((4,), jnp.int32), VMEM((32, 1024, 2, 128), BF16), VMEM((4, 8, 10, 16, 128), F32), VMEM((2, 8, 16, 128), F32),
            VMEM((32, 10, 4, 16, 128), F32), VMEM((32, 256, 128), BF16), VMEM((512, 256), F32),
            VMEM((4, 256, 128), F32), VMEM((4, 128, 128), F32), VMEM((4, 128, 128), F32), VMEM((16, 4, 8, 128), F32),
            VMEM((16, 128), F32), VMEM((16, 128), F32), VMEM((16, 128), F32), VMEM((16, 16, 128), F32), VMEM((4, 16, 128), F32),
            dma((5,)), dma((32,)), dma((4,)), dma((2, 5)), dma((2, 5)), dma((2,)), dma((2,)), dma((4,)), dma((4,)),
            dma((4,)), dma((4,)), dma((16, 4)), dma((16, 4)), dma, dma, dma((16,)), dma((16,)), dma((4,)), dma((4,)),
        ],
        compiler_params=pltpu.CompilerParams(collective_id=0, has_side_effects=True, vmem_limit_bytes=56 * MiB),
        name="main",
    )(shift_table, shift_ids, sources, kappa, mass, sketch.reshape(1024, 32, 2, 128))
    step, chunks = 2, 16
    out = sds((4, 32, 4, 16, 128), F32)
    return pl.pallas_call(
        functools.partial(output_kernel, chunks, step),
        out_shape=(out, out),
        in_specs=[hbm] * 2,
        out_specs=(hbm, hbm),
        scratch_shapes=[
            pltpu.SMEM((32, 128), F32), VMEM((32, 10, 4, 16, 128), F32), VMEM((4, 32, 4, 16, 128), F32),
            VMEM((4, 32, 4, 16, 128), F32), dma((chunks,)), dma((2, chunks)), dma,
        ],
        compiler_params=pltpu.CompilerParams(vmem_limit_bytes=60 * MiB),
        name="outputs",
    )(coef, fields)


def solution(mesh):
    placed = (
        P("shift", "dom", None, None), P("dom", None, None), P("dom", None, None), P(), P("shift"),
        P(None, "dom", None, None),
    )
    return jax.shard_map(
        on_device,
        mesh=mesh,
        in_specs=placed,
        out_specs=(P("shift", None, "dom", None, None), P("shift", None, "dom", None, None)),
        check_vma=False,
    )
```

```python
import functools
import jax
import jax.numpy as jnp
from jax import lax
from jax.experimental import pallas as pl
from jax.experimental.pallas import tpu as pltpu
from jax.sharding import PartitionSpec as P

F32 = jnp.float32
BF16 = jnp.bfloat16
CENTER = 2.25
K0 = 6.0 + CENTER
ORDER = (0, 1, 3, 4, 6, 7, 2, 5, 8, 9)
OWNER = (0, 1, 2, 2, 3, 3, 1, 2, 3, 3)
DEGREE = (0, 0, 0, 1, 0, 1, 1, 2, 2, 3)
LOWS = 6
VMEM = pltpu.VMEM
ANY = pl.ANY
MiB = 1024 * 1024


def rdma(src, dst, send, recv, where):
    return pltpu.make_async_remote_copy(
        src_ref=src, dst_ref=dst, send_sem=send, recv_sem=recv,
        device_id=where, device_id_type=pl.DeviceIdType.MESH,
    )


def signal(sem, where):
    pl.semaphore_signal(sem, inc=1, device_id=where, device_id_type=pl.DeviceIdType.MESH)


def neighbours(planes, i, masks):
    v = planes[i]
    first_y, last_y, first_z, last_z = masks
    beside = planes[i + 1] + planes[i - 1]
    beside = beside + jnp.where(first_y, 0.0, pltpu.roll(v, 1, 0)) + jnp.where(last_y, 0.0, pltpu.roll(v, 15, 0))
    return beside + jnp.where(first_z, 0.0, pltpu.roll(v, 1, 1)) + jnp.where(last_z, 0.0, pltpu.roll(v, 127, 1))


def make_masks():
    rows = lax.broadcasted_iota(jnp.int32, (16, 128), 0)
    lanes = lax.broadcasted_iota(jnp.int32, (16, 128), 1)
    return rows == 0, rows == 15, lanes == 0, lanes == 127


def fields_of(w, kap, mas, inside, masks):
    sixth = 1.0 / 6.0
    diag = [6.0 - kap[i] + CENTER * mas[i] for i in range(8)]

    def op(planes, i, k):
        return diag[k] * planes[i] - neighbours(planes, i, masks)

    z00, z01, p0, p1 = [], [], [], []
    for i in range(8):
        a = op(w, i + 1, i)
        b = mas[i] * w[i + 1]
        z00.append(a)
        z01.append(b)
        p0.append((a - K0 * w[i + 1]) * (sixth * inside[i]))
        p1.append((b - w[i + 1]) * sixth)
    z10, z11, z12, q0, q1, q2 = [], [], [], [], [], []
    for i in range(6):
        k = i + 1
        a = op(p0, k, k)
        b = op(p1, k, k) + mas[k] * p0[k]
        c = mas[k] * p1[k]
        z10.append(a)
        z11.append(b)
        z12.append(c)
        q0.append((a - K0 * p0[k]) * (sixth * inside[k]))
        q1.append((b - K0 * p1[k] - p0[k]) * (sixth * inside[k]))
        q2.append((c - p1[k]) * sixth)
    z20, z21, z22, z23 = [], [], [], []
    for i in range(4):
        k, n = i + 2, i + 1
        z20.append(op(q0, n, k))
        z21.append(op(q1, n, k) + mas[k] * q0[n])
        z22.append(op(q2, n, k) + mas[k] * q1[n])
        z23.append(mas[k] * q2[n])
    zs = [w[3:7], z00[2:6], z01[2:6], z10[1:5], z11[1:5], z12[1:5], z20, z21, z22, z23]
    return zs


def inside_of(d, doms):
    out = []
    for i in range(8):
        plane = d * 4 + (i - 2)
        ok = (plane >= 0) & (plane < doms * 4)
        out.append(jnp.where(ok, 1.0, 0.0).astype(F32))
    return out


def small_solve(gram, h):
    ridge = 0.001 * (gram(1, 1) + gram(2, 2) + gram(3, 3)) / 3.0 + 1.0
    e00, e11, e22 = gram(1, 1) + ridge, gram(2, 2) + ridge, gram(3, 3) + ridge
    e10, e20, e21 = gram(2, 1), gram(3, 1), gram(3, 2)
    l00 = jnp.sqrt(e00)
    l10 = e10 / l00
    l20 = e20 / l00
    l11 = jnp.sqrt(e11 - l10 * l10)
    l21 = (e21 - l20 * l10) / l11
    l22 = jnp.sqrt(e22 - l20 * l20 - l21 * l21)
    f0 = h(1) / l00
    f1 = (h(2) - l10 * f0) / l11
    f2 = (h(3) - l20 * f0 - l21 * f1) / l22
    c2 = f2 / l22
    c1 = (f1 - l21 * c2) / l11
    c0 = (f0 - l10 * c1 - l20 * c2) / l00
    return c0, c1, c2


def powers_of(t):
    return [jnp.ones_like(t), t, t * t, t * t * t]


def by_lane(shape, dim_size, values, group):
    lane = lax.broadcasted_iota(jnp.int32, shape, 1)
    which = (lane % 32) // group
    out = jnp.zeros(shape, F32)
    for j, v in enumerate(values):
        out = jnp.where(which == j, v, out)
    return out


def main_kernel(
    doms, zs, table_hbm, ids_hbm, src, kap, mas, s_ref, fields, coef,
    table, ids, buf, wide, cw, fb, gb, ob, part, r1, mine, r2, dm, dp, ds, rd, gall,
    loc, ssem, fsem, hs, hr, cs, cr, gs, gr, s1, e1, s2, e2, s3, e3, s4, e4, s5, e5,
):
    d, z = lax.axis_index("dom"), lax.axis_index("shift")
    up, down, far = lax.rem(z + 1, zs), lax.rem(z + zs - 1, zs), lax.rem(z + 2, zs)
    core, chip, chips = lax.rem(d, 2), d // 2, doms // 2
    partner = {"dom": d + 1 - 2 * core}
    has_l, has_r = d > 0, d < doms - 1
    copies = [
        pltpu.make_async_copy(src, wide.at[z, :, pl.ds(3, 4)], loc.at[0]),
        pltpu.make_async_copy(kap, cw.at[0, pl.ds(2, 4)], loc.at[1]),
        pltpu.make_async_copy(mas, cw.at[1, pl.ds(2, 4)], loc.at[2]),
    ]
    tables = [
        pltpu.make_async_copy(table_hbm, table, loc.at[3]),
        pltpu.make_async_copy(ids_hbm, ids, loc.at[4]),
    ]
    pairs = [pltpu.make_async_copy(s_ref.at[:, q], buf.at[q], ssem.at[q]) for q in range(32)]
    for c in copies + tables:
        c.start()
    bar = pltpu.get_barrier_semaphore()
    for k in range(1, doms):
        signal(bar, {"dom": lax.rem(d + k, doms)})
    for k in range(1, zs):
        signal(bar, {"shift": lax.rem(z + k, zs)})

    @pl.when(d == 0)
    def _():
        for g in range(4):
            for s in range(8):
                wide[g, s, 0:3] = jnp.zeros((3, 16, 128), F32)
        cw[:, 0:2] = jnp.zeros((2, 2, 16, 128), F32)

    @pl.when(d == doms - 1)
    def _():
        for g in range(4):
            for s in range(8):
                wide[g, s, 7:10] = jnp.zeros((3, 16, 128), F32)
        cw[:, 6:8] = jnp.zeros((2, 2, 16, 128), F32)

    for c in copies:
        c.wait()
    pl.semaphore_wait(bar, doms + zs - 2)

    def piece(n):
        g = (z, z, down, up, far)[n]
        return g, (pl.ds(4 * n, 4) if n < 2 else pl.ds(0, 8))

    def to_left(n):
        g, s = piece(n)
        return rdma(wide.at[g, s, pl.ds(3, 3)], wide.at[g, s, pl.ds(7, 3)], hs.at[0, n], hr.at[0, n], {"dom": d - 1})

    def to_right(n):
        g, s = piece(n)
        return rdma(wide.at[g, s, pl.ds(4, 3)], wide.at[g, s, pl.ds(0, 3)], hs.at[1, n], hr.at[1, n], {"dom": d + 1})

    def coeff_left():
        return rdma(cw.at[:, pl.ds(2, 2)], cw.at[:, pl.ds(6, 2)], cs.at[0], cr.at[0], {"dom": d - 1})

    def coeff_right():
        return rdma(cw.at[:, pl.ds(4, 2)], cw.at[:, pl.ds(0, 2)], cs.at[1], cr.at[1], {"dom": d + 1})

    def start_halo(g):
        @pl.when(has_l)
        def _():
            to_left(g).start()

        @pl.when(has_r)
        def _():
            to_right(g).start()

    def wait_halo(g):
        @pl.when(has_l)
        def _():
            to_right(g).wait_recv()

        @pl.when(has_r)
        def _():
            to_left(g).wait_recv()

    @pl.when(has_l)
    def _():
        coeff_left().start()

    @pl.when(has_r)
    def _():
        coeff_right().start()

    start_halo(0)
    start_halo(1)
    own = wide.at[z, :, pl.ds(3, 4)]
    for c in pairs:
        c.start()
    send_up = rdma(own, own, gs.at[0], gr.at[0], {"shift": up})
    send_down = rdma(own, own, gs.at[1], gr.at[1], {"shift": down})
    send_up.start()
    send_down.start()

    @pl.when(has_l)
    def _():
        coeff_right().wait_recv()

    @pl.when(has_r)
    def _():
        coeff_left().wait_recv()

    wait_halo(0)
    masks = make_masks()
    inside = inside_of(d, doms)

    def fields_for(g, sketched, begin=0, end=8):
        def one(s, carry):
            k = [cw[0, i] for i in range(8)]
            m = [cw[1, i] for i in range(8)]
            zf = fields_of([wide[g, s, i] for i in range(10)], k, m, inside, masks)
            at = g * 8 + s
            for n in range(10):
                for x in range(4):
                    fb[at, n, x] = zf[n][x]
            if sketched:
                col = pl.multiple_of(s * 16, 16)
                for x in range(4):
                    high = [zf[n][x] for n in ORDER]
                    low = [h - h.astype(BF16).astype(F32) for h in high[:LOWS]]
                    turned = jnp.transpose(jnp.stack(high + low, axis=0), (1, 0, 2)).astype(BF16)
                    for y in range(16):
                        gb[x * 8 + y // 2, pl.ds((y % 2) * 128 + col, 16), :] = turned[y]
            return carry

        lax.fori_loop(begin, end, one, 0)

    def save(g):
        return pltpu.make_async_copy(fb.at[pl.ds(g * 8, 8)], fields.at[pl.ds(g * 8, 8)], fsem.at[g])

    fields_for(z, True, 0, 4)
    wait_halo(1)
    fields_for(z, True, 4, 8)

    send_up.wait_recv()
    half_a = wide.at[down, pl.ds(0, 4), pl.ds(3, 4)]
    relay_up = rdma(half_a, half_a, gs.at[2], gr.at[2], {"shift": up})
    relay_up.start()
    send_down.wait_recv()
    half_b = wide.at[up, pl.ds(4, 4), pl.ds(3, 4)]
    relay_down = rdma(half_b, half_b, gs.at[3], gr.at[3], {"shift": down})
    relay_down.start()
    start_halo(2)
    start_halo(3)
    for c in tables + pairs:
        c.wait()
    save(z).start()

    rows = buf.reshape(32, 2048, 128)
    even = lax.broadcasted_iota(jnp.int32, (256, 128), 0) % 2 == 0
    other = pl.multiple_of((1 - core) * 128, 128)
    keep = pl.multiple_of(core * 128, 128)

    def swap(i):
        return rdma(part.at[i, pl.ds(other, 128)], r1.at[i], s1.at[i], e1.at[i], partner)

    def scatter(i, k):
        t = lax.rem(chip + k, chips)
        return rdma(
            mine.at[i, pl.ds(pl.multiple_of(t * 8, 8), 8)], r2.at[k, i], s2.at[k, i], e2.at[k, i], {"dom": 2 * t + core}
        )

    def spread(i):
        swap(i).wait_recv()
        mine[i] = part[i, pl.ds(keep, 128)] + r1[i]
        for k in (10, 2, 6, 14, 8, 9, 11, 5, 7, 13, 15, 1, 3, 4, 12):
            scatter(i, k).start()

    def stage(i, carry):
        rhs = jnp.concatenate([gb[q] for q in range(32)], axis=1)
        at, bt = pl.multiple_of(i * 256, 256), pl.multiple_of(i * 256 + 1024, 256)
        lhs = jnp.concatenate(
            [jnp.concatenate([rows[q, pl.ds(at, 256), :], rows[q, pl.ds(bt, 256), :]], axis=0) for q in range(32)], axis=1
        )
        ob[...] = lax.dot_general(lhs, rhs, (((1,), (1,)), ((), ())), preferred_element_type=F32)
        a, b = ob[0:256], ob[256:512]
        xa = a[:, :128] + pltpu.roll(a[:, 128:], 255, 0)
        xb = b[:, 128:] + pltpu.roll(b[:, :128], 1, 0)
        part[i] = jnp.where(even, xa, xb)
        swap(i).start()

        @pl.when(i > 0)
        def _():
            spread(i - 1)

        return carry

    lax.fori_loop(0, 4, stage, 0)
    spread(3)
    relay_up.wait_recv()
    relay_down.wait_recv()
    start_halo(4)
    wait_halo(2)
    fields_for(down, False)

    v = []
    for i in range(4):
        total = mine[i, pl.ds(pl.multiple_of(chip * 8, 8), 8)]
        for k in range(1, chips):
            scatter(i, k).wait_recv()
            total = total + r2[k, i]
        v.append(total)
    v = jnp.concatenate(v, axis=0)
    lane = lax.broadcasted_iota(jnp.int32, (32, 128), 1) % 16
    v = v + jnp.where(lane < LOWS, pltpu.roll(v, 118, 1), 0.0)
    v = jnp.where(lane < 10, v, 0.0)
    full = lax.dot_general(v, v, (((0,), (0,)), ((), ())), precision=lax.Precision.HIGHEST, preferred_element_type=F32)
    owner = lax.broadcasted_iota(jnp.int32, (16, 128), 1) // 16
    diag = jnp.zeros((16, 128), F32)
    for s in range(8):
        diag = jnp.where(owner == s, full[16 * s : 16 * s + 16], diag)
    dm[...] = diag
    pair = rdma(dm, dp, s3, e3, partner)
    pair.start()
    save(down).start()
    pair.wait_recv()
    ds[...] = diag + dp[...]
    sums = []
    for k in range(1, chips):
        c = rdma(ds, rd.at[k], s4.at[k], e4.at[k], {"dom": 2 * lax.rem(chip + k, chips) + core})
        c.start()
        sums.append(c)
    wait_halo(3)
    fields_for(up, False)
    total = ds[...]
    for k, c in zip(range(1, chips), sums):
        c.wait_recv()
        total = total + rd[k]
    gall[z] = total
    tail = []
    for k in range(1, zs):
        c = rdma(gall.at[z], gall.at[z], s5.at[k], e5.at[k], {"shift": lax.rem(z + k, zs)})
        c.start()
        tail.append(c)
    save(up).start()
    wait_halo(4)
    fields_for(far, False)
    save(far).start()

    shifts = [table[ids[j]] - CENTER for j in range(4)]
    r = lax.broadcasted_iota(jnp.int32, (128, 128), 0)
    l = lax.broadcasted_iota(jnp.int32, (128, 128), 1)
    tw = by_lane((128, 128), 128, shifts, 8)
    pw = powers_of(tw)
    fold = jnp.zeros((128, 128), F32)
    for n in range(10):
        hit = (r % 16 == n) & (r // 16 == l % 8) & (l // 32 == OWNER[n])
        fold = jnp.where(hit, pw[DEGREE[n]], fold)
    for c in tail:
        c.wait_recv()
    mixed = lax.dot_general(
        gall[...].reshape(64, 128), fold, (((1,), (0,)), ((), ())), precision=lax.Precision.HIGHEST, preferred_element_type=F32
    )
    t = by_lane((1, 128), 128, shifts, 8)
    pt = powers_of(t)
    lines = []
    for i in range(1, 4):
        per_z = []
        for g in range(4):
            acc = jnp.zeros((1, 128), F32)
            for n in range(10):
                if OWNER[n] == i:
                    acc = acc + pt[DEGREE[n]] * mixed[g * 16 + n : g * 16 + n + 1]
            per_z.append(acc)
        lines.append(jnp.concatenate(per_z + per_z, axis=0))

    def gram(i, k):
        return lines[i - 1] if k == 0 else pltpu.roll(lines[i - 1], 128 - 32 * k, 1)

    c0, c1, c2 = small_solve(gram, lambda i: gram(i, 0))
    t = by_lane((8, 128), 128, shifts, 8)
    center = K0 + t
    sixth = 1.0 / 6.0
    e = c1 - c2 * center * sixth
    out = [c0, c0 * t, c1, c1 * t, c1 * t * t, c2, c2 * t, c2 * t * t, c2 * t * t * t]
    out += [c0 - e * center * sixth, e * sixth, e * t * sixth, c2 * sixth, c2 * t * sixth, c2 * t * t * sixth, c2]
    quarter = lax.broadcasted_iota(jnp.int32, (8, 128), 1) // 32
    for n4 in range(4):
        acc = jnp.zeros((8, 128), F32)
        for k in range(4):
            c = out[n4 * 4 + k]
            acc = jnp.where(quarter == k, c if k == 0 else pltpu.roll(c, 32 * k, 1), acc)
        coef[n4 * 8 : n4 * 8 + 8] = acc

    for i in range(4):
        swap(i).wait_send()
        for k in range(1, chips):
            scatter(i, k).wait_send()
    for c in [pair, send_up, send_down, relay_up, relay_down] + sums + tail:
        c.wait_send()

    @pl.when(has_l)
    def _():
        coeff_left().wait_send()
        for n in range(5):
            to_left(n).wait_send()

    @pl.when(has_r)
    def _():
        coeff_right().wait_send()
        for n in range(5):
            to_right(n).wait_send()

    for g in range(4):
        save(g).wait()


def output_kernel(chunks, step, coef_hbm, fields, sol, res, coef, fin, so, ro, isem, osem, csem):
    def take(i):
        part = pl.ds(i * step, step)
        return pltpu.make_async_copy(fields.at[part], fin.at[part], isem.at[i])

    def put(i):
        part = pl.ds(i * step, step)
        return [
            pltpu.make_async_copy(so.at[:, part], sol.at[:, part], osem.at[0, i]),
            pltpu.make_async_copy(ro.at[:, part], res.at[:, part], osem.at[1, i]),
        ]

    ahead = 4
    first = pltpu.make_async_copy(coef_hbm, coef, csem)
    first.start()
    for i in range(ahead):
        take(i).start()
    first.wait()

    def chunk(i, carry):
        take(i).wait()

        @pl.when(i + ahead < chunks)
        def _():
            take(i + ahead).start()

        def one(k, carry):
            b = i * step + k
            g, s = b // 8, lax.rem(b, 8)
            for j in range(4):
                c = [coef[(n // 4) * 8 + g, (n % 4) * 32 + j * 8 + s] for n in range(15)]
                for x in range(4):
                    f = [fin[b, n, x] for n in range(10)]
                    u = c[9] * f[0]
                    for n in range(1, 6):
                        u = u + c[9 + n] * f[n]
                    r = f[0] - c[0] * f[1]
                    for n in range(1, 9):
                        r = r - c[n] * f[n + 1]
                    so[j, b, x] = u
                    ro[j, b, x] = r
            return carry

        lax.fori_loop(0, step, one, 0)

        @pl.when(i > 0)
        def _():
            for c in put(i - 1):
                c.start()

        return carry

    lax.fori_loop(0, chunks, chunk, 0)
    for c in put(chunks - 1):
        c.start()
    for i in range(chunks):
        for c in put(i):
            c.wait()


def on_device(sources, kappa, mass, shift_table, shift_ids, sketch):
    doms, zs = lax.axis_size("dom"), lax.axis_size("shift")
    sds = jax.ShapeDtypeStruct
    dma = pltpu.SemaphoreType.DMA
    hbm = pl.BlockSpec(memory_space=ANY)
    fields, coef = pl.pallas_call(
        functools.partial(main_kernel, doms, zs),
        out_shape=(sds((32, 10, 4, 16, 128), F32), sds((32, 128), F32)),
        in_specs=[hbm] * 6,
        out_specs=(hbm, pl.BlockSpec(memory_space=VMEM)),
        scratch_shapes=[
            pltpu.SMEM((64,), F32), pltpu.SMEM((4,), jnp.int32), VMEM((32, 1024, 2, 128), BF16), VMEM((4, 8, 10, 16, 128), F32), VMEM((2, 8, 16, 128), F32),
            VMEM((32, 10, 4, 16, 128), F32), VMEM((32, 256, 128), BF16), VMEM((512, 256), F32),
            VMEM((4, 256, 128), F32), VMEM((4, 128, 128), F32), VMEM((4, 128, 128), F32), VMEM((16, 4, 8, 128), F32),
            VMEM((16, 128), F32), VMEM((16, 128), F32), VMEM((16, 128), F32), VMEM((16, 16, 128), F32), VMEM((4, 16, 128), F32),
            dma((5,)), dma((32,)), dma((4,)), dma((2, 5)), dma((2, 5)), dma((2,)), dma((2,)), dma((4,)), dma((4,)),
            dma((4,)), dma((4,)), dma((16, 4)), dma((16, 4)), dma, dma, dma((16,)), dma((16,)), dma((4,)), dma((4,)),
        ],
        compiler_params=pltpu.CompilerParams(collective_id=0, has_side_effects=True, vmem_limit_bytes=56 * MiB),
        name="main",
    )(shift_table, shift_ids, sources, kappa, mass, sketch.reshape(1024, 32, 2, 128))
    step, chunks = 2, 16
    out = sds((4, 32, 4, 16, 128), F32)
    return pl.pallas_call(
        functools.partial(output_kernel, chunks, step),
        out_shape=(out, out),
        in_specs=[hbm] * 2,
        out_specs=(hbm, hbm),
        scratch_shapes=[
            pltpu.SMEM((32, 128), F32), VMEM((32, 10, 4, 16, 128), F32), VMEM((4, 32, 4, 16, 128), F32),
            VMEM((4, 32, 4, 16, 128), F32), dma((chunks,)), dma((2, chunks)), dma,
        ],
        compiler_params=pltpu.CompilerParams(vmem_limit_bytes=60 * MiB),
        name="outputs",
    )(coef, fields)


def solution(mesh):
    placed = (
        P("shift", "dom", None, None), P("dom", None, None), P("dom", None, None), P(), P("shift"),
        P(None, "dom", None, None),
    )
    return jax.shard_map(
        on_device,
        mesh=mesh,
        in_specs=placed,
        out_specs=(P("shift", None, "dom", None, None), P("shift", None, "dom", None, None)),
        check_vma=False,
    )
```
